512 devices in a mesh: resp: 64 (over y, z), head: 8 (over x, core).
Axes of the slice: x: 4, y: 8, z: 8, core: 2. Of those that a mesh axis runs over, the one named last changes fastest.
Arguments:
- queries: bfloat16 [8192, 24576], P('resp', 'head'), may hold values from -8 to 8
- resp_latent: bfloat16 [8192, 576], P('resp'), may hold values from -8 to 8
- prompt_latent: bfloat16 [64, 128, 576], P('resp'), may hold values from -6 to 6
- up_keys: bfloat16 [128, 128, 512], P('head', None, 'resp'), may hold values from -0.5 to 0.5
- up_values: bfloat16 [128, 512, 128], P('head', 'resp'), may hold values from -0.25 to 0.25
- cotangent: bfloat16 [8192, 16384], P('resp', 'head'), may hold values from -6 to 6
- prompt_len: int32 [32], replicated, may hold values from 32 to 128
- resp_len: int32 [128], replicated, may hold values from 16 to 64
- resp_count: int32 [32], replicated, may hold values from 1 to 8, 128 in all
- owner: int32 [32], replicated, may hold values from 0 to 63, as said below
Outputs:
- attended: bfloat16 [8192, 16384], P('resp', 'head')
- grad_queries: bfloat16 [8192, 24576], P('resp', 'head')
- grad_response: float32 [8192, 576], P('resp', 'head')
- grad_prompt: float32 [64, 128, 576], P('resp', None, 'head')
The draws below stay inside these ranges and needn't reach their ends.
Inputs may be any that keep to these rules, and one draw needn't show every extreme that they name: Distinct slots; prompt p's cache is prompt_latent[owner[p]]. `resp_count`: every prompt has at least one response; they sum to 128.
All inputs are finite; a program needn't handle non-finite values.
Results may differ from the reference program's by a relative error of at most 0.014.
Values may be sent and summed in bfloat16 or wider, within the bound.
No kernel may reach another device: no remote copies, remote signals or barrier semaphores. Data moves between devices by JAX's collectives and lax.ppermute only.
A program may use at most 64 MiB of HBM per device.

```python
import math
import jax
import jax.numpy as jnp
import numpy as np
from jax import lax

HEADS = 128
D_LAT = 512
D_ROPE = 64
D_NOPE = 128
D_VAL = 128
RL = 64
PLEN = 128
NPROMPT = 32
NRESP = 128
MOST = 8
TOKENS = 8192
N_RESP = 64


def draw_owner(key, part):
    shuffled = jax.random.permutation(jax.random.fold_in(key, 7), N_RESP)
    return shuffled[:NPROMPT].astype(jnp.int32)


def draw_queries(key, part):
    query_width = D_NOPE + D_ROPE
    sampled = jax.random.truncated_normal(jax.random.fold_in(key, 1), -6.0, 6.0, (TOKENS, HEADS, query_width), jnp.float32)
    return sampled.reshape(TOKENS, HEADS * query_width).astype(jnp.bfloat16)


def draw_resp_latent(key, part):
    sampled = jax.random.truncated_normal(jax.random.fold_in(key, 2), -6.0, 6.0, (TOKENS, D_LAT + D_ROPE), jnp.float32)
    return sampled.astype(jnp.bfloat16)


def with_ends(drawn, own_key, low, top_value):
    index_at = [jax.random.randint(jax.random.fold_in(own_key, axis), (), 0, length) for axis, length in enumerate(drawn.shape)]
    widest = drawn.shape.index(max(drawn.shape))
    neighbour = index_at[:widest] + [(index_at[widest] + 1) % drawn.shape[widest]] + index_at[widest + 1:]
    return drawn.at[tuple(index_at)].set(low).at[tuple(neighbour)].set(top_value)


def shard_levels(key, shape, pieces, least, top_value):
    def one(dim, shards_of):
        draws = jax.random.uniform(jax.random.fold_in(jax.random.fold_in(key, 6), dim), (shards_of,), jnp.float32, least / len(pieces), top_value / len(pieces))
        return jnp.repeat(jnp.exp(draws), shape[dim] // shards_of).reshape((-1,) + (1,) * (len(shape) - dim - 1))

    factor_of = one(*pieces[0])
    for cut in pieces[1:]:
        factor_of = factor_of * one(*cut)
    return factor_of


def length_profile(count, total, reach, slope):
    portions = [(1 << 20) // math.isqrt(standing ** slope) + 1 for standing in range(2, count + 1)]
    rest, given = total - reach - (count - 1), [1] * (count - 1)
    while rest > 0:
        movable = [i for i in range(count - 1) if given[i] < reach]
        pool, left = sum([portions[i] for i in movable]), rest
        for i in movable:
            addition = min(reach - given[i], max(1, left * portions[i] // pool), rest)
            given[i] = given[i] + addition
            rest = rest - addition
    return np.array([reach] + given)


def uneven(rng, number_of, total, most, lean):
    if number_of == 2:
        one = jax.random.randint(rng, (), max(1, total - most), min(most, total - 1) + 1)
        return jnp.stack([one, total - one])
    lengths = jnp.asarray(length_profile(number_of, total, most, lean), jnp.int32)
    pairs = (number_of - 1) // 2
    source_of, taker = lengths[1:1 + 2 * pairs:2], lengths[2:2 + 2 * pairs:2]
    room = jnp.minimum(source_of - 1, most - taker)
    shifted = jax.random.randint(jax.random.fold_in(rng, 1), (pairs,), 0, 1 << 20) % (room + 1)
    lengths = lengths.at[1:1 + 2 * pairs:2].set(source_of - shifted).at[2:2 + 2 * pairs:2].set(taker + shifted)
    return lengths[jax.random.permutation(jax.random.fold_in(rng, 2), number_of)]


def gaussian(rng, dims, scale, reach, shards=(), kind=jnp.bfloat16):
    result = scale * jax.random.normal(rng, dims, jnp.float32)
    if shards:
        result = result * shard_levels(rng, dims, shards, -0.22, 0.18)
    return jnp.clip(result, -reach, reach).astype(kind)


def setup_inputs(seed: int = 0) -> dict:
    arg_keys = jax.random.split(jax.random.key(seed), 11)
    queries = draw_queries(jax.random.fold_in(arg_keys[10], 71), 0)
    resp_latent = draw_resp_latent(jax.random.fold_in(arg_keys[10], 71), 0)
    prompt_latent = gaussian(arg_keys[2], (N_RESP, PLEN, D_LAT + D_ROPE), 1.0, 6.0, ((0, 64),))
    up_keys = gaussian(arg_keys[3], (HEADS, D_NOPE, D_LAT), D_NOPE ** -0.5, 0.5, ((0, 8), (2, 64)))
    up_values = gaussian(arg_keys[4], (HEADS, D_LAT, D_VAL), D_LAT ** -0.5, 0.25, ((0, 8), (1, 64)))
    cotangent = gaussian(arg_keys[5], (TOKENS, HEADS * D_VAL), 1.0, 6.0, ((0, 64), (1, 8)))
    prompt_len = with_ends(jax.random.randint(arg_keys[6], (NPROMPT,), PLEN // 4, PLEN + 1), jax.random.fold_in(arg_keys[6], 1), PLEN // 4, PLEN).astype(jnp.int32)
    resp_len = with_ends(jax.random.randint(arg_keys[7], (NRESP,), RL // 4, RL + 1), jax.random.fold_in(arg_keys[7], 1), RL // 4, RL).astype(jnp.int32)
    resp_count = uneven(arg_keys[8], NPROMPT, NRESP, MOST, 2).astype(jnp.int32)
    owner = draw_owner(jax.random.fold_in(arg_keys[10], 71), 0)
    return {"queries": queries, "resp_latent": resp_latent, "prompt_latent": prompt_latent, "up_keys": up_keys, "up_values": up_values, "cotangent": cotangent, "prompt_len": prompt_len, "resp_len": resp_len, "resp_count": resp_count, "owner": owner}


def product(form, left, right):
    return jnp.einsum(form, left.astype(jnp.float32), right.astype(jnp.float32))

def attend(queries, key_rows, key_valid, row_live, cotangent, up_keys, up_values):
    head_count, nope_width, latent_width = up_keys.shape
    row_count = queries.shape[0]
    split_query = queries.reshape(row_count, head_count, -1)
    score_scale = 1.0 / math.sqrt(split_query.shape[2])
    query_latent = product('thn,hnc->thc', split_query[:, :, :nope_width], up_keys).astype(jnp.bfloat16)
    query_full = jnp.concatenate([query_latent, split_query[:, :, nope_width:]], axis=2)
    scores = product('thc,kc->thk', query_full, key_rows) * score_scale
    scores = jnp.where(key_valid[:, None, :], scores, -jnp.inf)
    row_max = lax.optimization_barrier(jnp.max(scores, axis=2, keepdims=True))
    expo = jnp.exp(scores - row_max)
    weights = expo / lax.optimization_barrier(jnp.sum(expo, axis=2, keepdims=True))
    weights_bf = weights.astype(jnp.bfloat16)
    value_rows = key_rows[:, :latent_width]
    latent_out = product('thk,kc->thc', weights_bf, value_rows).astype(jnp.bfloat16)
    attended = product('thc,hcv->thv', latent_out, up_values) * row_live[:, None, None]
    grad_out = cotangent.reshape(row_count, head_count, -1)
    grad_latent = (product('thv,hcv->thc', grad_out, up_values) * row_live[:, None, None]).astype(jnp.bfloat16)
    grad_weights = product('thc,kc->thk', grad_latent, value_rows)
    inner = lax.optimization_barrier(jnp.sum(weights * grad_weights, axis=2, keepdims=True))
    grad_scores = (weights * (grad_weights - inner) * score_scale).astype(jnp.bfloat16)
    grad_full = product('thk,kc->thc', grad_scores, key_rows)
    grad_nope = product('thc,hnc->thn', grad_full[:, :, :latent_width].astype(jnp.bfloat16), up_keys)
    grad_query = jnp.concatenate([grad_nope, grad_full[:, :, latent_width:]], axis=2)
    grad_key = product('thk,thc->kc', grad_scores, query_full)
    grad_value = product('thk,thc->kc', weights_bf, grad_latent)
    grad_key = grad_key + jnp.pad(grad_value, ((0, 0), (0, key_rows.shape[1] - latent_width)))
    return (attended.reshape(row_count, -1).astype(jnp.bfloat16), grad_query.reshape(row_count, -1).astype(jnp.bfloat16), grad_key)

def reference(queries, resp_latent, prompt_latent, up_keys, up_values, cotangent, prompt_len, resp_len, resp_count, owner):
    resp_total = resp_len.shape[0]
    row_count = queries.shape[0] // resp_total
    prompt_rows = prompt_latent.shape[1]
    starts = jnp.cumsum(resp_count) - resp_count
    numbers = jnp.arange(resp_total, dtype=jnp.int32)
    prompt_of = lax.optimization_barrier(jnp.sum((starts[None, :] <= numbers[:, None]).astype(jnp.int32), axis=1)) - 1
    chosen = prompt_of[:, None] == jnp.arange(prompt_len.shape[0], dtype=jnp.int32)[None, :]
    slot_of = lax.optimization_barrier(jnp.sum(jnp.where(chosen, owner[None, :], 0), axis=1)).astype(jnp.int32)
    plen_of = lax.optimization_barrier(jnp.sum(jnp.where(chosen, prompt_len[None, :], 0), axis=1)).astype(jnp.int32)
    positions = jnp.arange(row_count, dtype=jnp.int32)
    prompt_pos = jnp.arange(prompt_rows, dtype=jnp.int32)
    causal = positions[:, None] >= positions[None, :]

    def one_response(carry, number):
        start = (number * row_count).astype(jnp.int32)
        query_rows = lax.dynamic_slice_in_dim(queries, start, row_count, 0)
        own_rows = lax.dynamic_slice_in_dim(resp_latent, start, row_count, 0)
        grad_rows = lax.dynamic_slice_in_dim(cotangent, start, row_count, 0)
        slot = slot_of[number]
        prompt_rows_now = lax.dynamic_index_in_dim(prompt_latent, slot, 0, keepdims=False)
        key_rows = jnp.concatenate([prompt_rows_now, own_rows], axis=0)
        prompt_ok = jnp.broadcast_to(prompt_pos[None, :] < plen_of[number], (row_count, prompt_rows))
        key_valid = jnp.concatenate([prompt_ok, causal], axis=1)
        row_live = (positions < resp_len[number]).astype(jnp.float32)
        attended, grad_query, grad_key = attend(query_rows, key_rows, key_valid, row_live, grad_rows, up_keys, up_values)
        carry = carry.at[slot].add(grad_key[:prompt_rows])
        return (carry, (attended, grad_query, grad_key[prompt_rows:]))
    empty = jnp.zeros(prompt_latent.shape, jnp.float32)
    grad_prompt, (attended, grad_queries, grad_response) = lax.scan(one_response, empty, numbers)
    return (attended.reshape(queries.shape[0], -1), grad_queries.reshape(queries.shape[0], -1), grad_response.reshape(queries.shape[0], -1), grad_prompt)
```

```python
import functools
import math

import jax
import jax.numpy as jnp
from jax import lax
from jax.experimental import pallas as pl
from jax.experimental.pallas import tpu as pltpu
from jax.sharding import PartitionSpec as P

F32, BF16 = jnp.float32, jnp.bfloat16
STEP_HEADS = 4


def dot(left, right, dims=((1,), (0,))):
    return lax.dot_general(left, right, (dims, ((), ())), preferred_element_type=F32)


NT, TN = ((1,), (1,)), ((0,), (0,))


def attend_kernel(
    sizes, plen, rlen, q_ref, ct_ref, wv_ref, wk_ref, kp_ref, ko_ref,
    out_ref, gq_ref, gk_ref, k_s, kt_s, qf_s, gl_s, lo_s, gf_s, acc_s,
):
    parts, rows, heads, nope, rope, val, lat, prows = sizes
    full, width, wide = lat + rope, nope + rope, k_s.shape[2]
    tokens = parts * rows
    step = pl.program_id(0)
    scale = 1.0 / math.sqrt(width)

    @pl.when(step == 0)
    def _():
        own = ko_ref[...]
        own_rows = jnp.transpose(own)
        for r in range(parts):
            cols = kp_ref[r]
            kt_s[r] = jnp.zeros(kt_s.shape[1:], BF16)
            kt_s[r, :full, :prows] = cols
            kt_s[r, :full, prows:] = own
            k_s[r] = jnp.zeros(k_s.shape[1:], BF16)
            k_s[r, :prows, :full] = jnp.transpose(cols)
            k_s[r, prows:, :full] = own_rows
        qf_s[...] = jnp.zeros_like(qf_s)
        gl_s[...] = jnp.zeros_like(gl_s)
        acc_s[...] = jnp.zeros_like(acc_s)

    wv = wv_ref[...]
    wk = wk_ref[...]
    q = q_ref[...]
    ct = ct_ref[...]
    spot = lax.broadcasted_iota(jnp.int32, (tokens, 1), 0)
    live = jnp.zeros((tokens, 1), F32)
    for r in range(parts):
        alive = (spot >= r * rows) & (spot < r * rows + rlen[r])
        live = jnp.where(alive, 1.0, live)
    for j in range(heads):
        wk_j = wk[:, j * nope : (j + 1) * nope]
        wv_j = wv[:, j * val : (j + 1) * val]
        at = j * width
        q_lat = dot(q[:, at : at + nope], wk_j, NT).astype(BF16)
        q_rope = q[:, at + nope : at + width]
        g_lat = (dot(ct[:, j * val : (j + 1) * val], wv_j, NT) * live).astype(BF16)
        for r in range(parts):
            here = slice(r * rows, (r + 1) * rows)
            there = slice(j * rows, (j + 1) * rows)
            qf_s[r, there, :lat] = q_lat[here]
            qf_s[r, there, lat:full] = q_rope[here]
            gl_s[r, there, :lat] = g_lat[here]
    block = heads * rows
    keys = kt_s.shape[2]
    for r in range(parts):
        qf, gl = qf_s[r], gl_s[r]
        scores = dot(qf, kt_s[r]) * scale
        place = lax.broadcasted_iota(jnp.int32, (block, keys), 0) % rows
        key = lax.broadcasted_iota(jnp.int32, (block, keys), 1)
        own = key - (prows + r * rows)
        valid = (key < plen[r]) | ((own >= 0) & (own <= place))
        scores = jnp.where(valid, scores, -jnp.inf)
        expo = jnp.exp(scores - jnp.max(scores, axis=1, keepdims=True))
        weights = expo / jnp.sum(expo, axis=1, keepdims=True)
        weights_bf = weights.astype(BF16)
        lo_s[r] = dot(weights_bf, k_s[r, :, :lat]).astype(BF16)
        grad_w = dot(gl[:, :lat], kt_s[r, :lat])
        inner = jnp.sum(weights * grad_w, axis=1, keepdims=True)
        grad_s = (weights * (grad_w - inner) * scale).astype(BF16)
        gf_s[r] = dot(grad_s, k_s[r]).astype(BF16)
        both = jnp.concatenate([grad_s, weights_bf], axis=0)
        rest = jnp.concatenate([qf, gl], axis=0)
        grad_k = dot(both, rest, TN)
        acc_s[r * prows : (r + 1) * prows] += grad_k[:prows]
        acc_s[parts * prows :] += grad_k[prows:]
    pieces = []
    for j in range(heads):
        wk_j = wk[:, j * nope : (j + 1) * nope]
        wv_j = wv[:, j * val : (j + 1) * val]
        there = slice(j * rows, (j + 1) * rows)
        low = jnp.concatenate([lo_s[r, there] for r in range(parts)], axis=0)
        gf = jnp.concatenate([gf_s[r, there] for r in range(parts)], axis=0)
        out_ref[:, j * val : (j + 1) * val] = (dot(low, wv_j) * live).astype(BF16)
        pieces += [dot(gf[:, :lat], wk_j).astype(BF16), gf[:, lat:full]]
    gq_ref[...] = jnp.concatenate(pieces, axis=1)

    @pl.when(step == pl.num_programs(0) - 1)
    def _():
        gk_ref[...] = jnp.transpose(acc_s[...])[:full].astype(BF16)


def attend(plen, rlen, queries, cotangent, weights, k_prompt, k_own, nope):
    parts, full, prows = k_prompt.shape
    lat = weights.shape[0]
    rope = full - lat
    width = nope + rope
    tokens = queries.shape[0]
    heads = queries.shape[1] // width
    val = cotangent.shape[1] // heads
    rows = tokens // parts
    hs = STEP_HEADS
    steps = heads // hs
    sizes = (parts, rows, hs, nope, rope, val, lat, prows)
    wide = -(-full // 128) * 128
    keys = prows + tokens
    whole = lambda *shape: pl.BlockSpec(shape, lambda i, *_: (0,) * len(shape))
    flops = 2 * tokens * heads * (4 * lat * nope + keys * (3 * full + 3 * lat))
    return pl.pallas_call(
        functools.partial(attend_kernel, sizes),
        out_shape=(
            jax.ShapeDtypeStruct((tokens, heads * val), BF16),
            jax.ShapeDtypeStruct((tokens, heads * width), BF16),
            jax.ShapeDtypeStruct((full, parts * prows + tokens), BF16),
        ),
        grid_spec=pltpu.PrefetchScalarGridSpec(
            num_scalar_prefetch=2,
            grid=(steps,),
            in_specs=[
                pl.BlockSpec((tokens, hs * width), lambda i, *_: (0, i)),
                pl.BlockSpec((tokens, hs * val), lambda i, *_: (0, i)),
                pl.BlockSpec((lat, hs * val), lambda i, *_: (0, i)),
                pl.BlockSpec((lat, hs * nope), lambda i, *_: (0, i + steps)),
                whole(parts, full, prows),
                whole(full, tokens),
            ],
            out_specs=[
                pl.BlockSpec((tokens, hs * val), lambda i, *_: (0, i)),
                pl.BlockSpec((tokens, hs * width), lambda i, *_: (0, i)),
                whole(full, parts * prows + tokens),
            ],
            scratch_shapes=[
                pltpu.VMEM((parts, keys, wide), BF16),
                pltpu.VMEM((parts, wide, keys), BF16),
                pltpu.VMEM((parts, hs * rows, wide), BF16),
                pltpu.VMEM((parts, hs * rows, wide), BF16),
                pltpu.VMEM((parts, hs * rows, lat), BF16),
                pltpu.VMEM((parts, hs * rows, wide), BF16),
                pltpu.VMEM((parts * prows + tokens, wide), F32),
            ],
        ),
        compiler_params=pltpu.CompilerParams(
            dimension_semantics=("arbitrary",), vmem_limit_bytes=48 << 20
        ),
        cost_estimate=pl.CostEstimate(
            flops=flops, transcendentals=tokens * heads * keys, bytes_accessed=8 << 20
        ),
        name="attend",
    )(plen, rlen, queries, cotangent, weights, weights, k_prompt, k_own)


def side_of(axis):
    return math.isqrt(lax.axis_size(axis))


def rows_of(side):
    return [[y * side + z for z in range(side)] for y in range(side)]


def columns_of(side):
    return [[y * side + z for y in range(side)] for z in range(side)]


def exchange(tiles, axis, groups=None):
    return lax.all_to_all(tiles, axis, 0, 0, axis_index_groups=groups, tiled=True)


def to_all(array, count, axis, groups=None):
    return exchange(jnp.broadcast_to(array, (count, *array.shape)), axis, groups)


def body(
    queries,
    resp_latent,
    prompt_latent,
    up_keys,
    up_values,
    cotangent,
    prompt_len,
    resp_len,
    resp_count,
    owner,
):
    head_devices = lax.axis_size("head")
    side = side_of("resp")
    along_z, along_y = rows_of(side), columns_of(side)
    my_index = lax.axis_index("resp")
    my_y, my_z = my_index // side, my_index % side
    head_index = lax.axis_index("head")
    heads, nope, lat_piece = up_keys.shape
    val = up_values.shape[2]
    resp_total = resp_len.shape[0]
    per_device = resp_total // lax.axis_size("resp")
    _, prompt_rows, full = prompt_latent.shape
    share = full // head_devices

    tiles = jnp.concatenate([up_values, jnp.swapaxes(up_keys, 1, 2)], axis=0)
    flat = tiles.reshape(-1, tiles.shape[2])
    weight_rows = flat.shape[0]
    cols = jnp.swapaxes(prompt_latent[0], 0, 1)
    cols = lax.dynamic_slice_in_dim(cols, head_index * share, share, 0)
    got = to_all(jnp.concatenate([flat, cols], axis=0), side, "resp", along_z)
    stripes = got[:, :weight_rows].reshape(side, *tiles.shape)
    stripes = jnp.moveaxis(stripes, 2, 1).reshape(side * lat_piece, -1)
    weights = lax.all_gather(
        stripes, "resp", axis=0, tiled=True, axis_index_groups=along_y
    )
    row_prompts = got[:, weight_rows:]

    starts = jnp.cumsum(resp_count) - resp_count
    numbers = jnp.arange(resp_total, dtype=jnp.int32)
    prompt_of = jnp.sum((starts[None, :] <= numbers[:, None]).astype(jnp.int32), axis=1) - 1
    chosen = prompt_of[:, None] == jnp.arange(prompt_len.shape[0], dtype=jnp.int32)[None, :]
    slot_of = jnp.sum(jnp.where(chosen, owner[None, :], 0), axis=1)
    plen_of = jnp.sum(jnp.where(chosen, prompt_len[None, :], 0), axis=1)
    first = my_index * per_device
    plen_mine = lax.dynamic_slice_in_dim(plen_of, first, per_device)
    rlen_mine = lax.dynamic_slice_in_dim(resp_len, first, per_device)
    slots_mine = lax.dynamic_slice_in_dim(slot_of, first, per_device)

    by_place = slot_of.reshape(side, side, per_device)
    in_column = lax.dynamic_index_in_dim(by_place, my_z, 1, keepdims=False)
    wanted = jnp.take(row_prompts, (in_column % side).reshape(-1), axis=0)
    wanted = wanted.reshape(side, per_device, share, prompt_rows)
    arrived = exchange(wanted, "resp", along_y)
    mine = (slots_mine // side)[None, :] == jnp.arange(side, dtype=jnp.int32)[:, None]
    fetched = jnp.sum(
        jnp.where(mine[:, :, None, None], arrived, 0).astype(F32), axis=0
    ).astype(BF16)
    k_prompt = to_all(fetched, head_devices, "head")
    k_prompt = jnp.moveaxis(k_prompt, 0, 1).reshape(per_device, full, prompt_rows)
    k_own = jnp.swapaxes(resp_latent, 0, 1)

    attended, grad_query, grad_key = attend(
        plen_mine, rlen_mine, queries, cotangent, weights, k_prompt, k_own, nope
    )
    by_head = exchange(grad_key.reshape(head_devices, share, -1), "head")
    summed = jnp.sum(by_head.astype(F32), axis=0)
    split = per_device * prompt_rows
    grad_own = jnp.swapaxes(summed[:, split:], 0, 1)
    grad_prompt = summed[:, :split].astype(BF16)
    in_row = to_all(grad_prompt, side, "resp", along_z)
    row_slots = lax.dynamic_index_in_dim(by_place, my_y, 0, keepdims=False)
    takers = jnp.arange(side, dtype=jnp.int32) * side + my_z
    in_row = in_row.reshape(side, share, per_device, prompt_rows).astype(F32)
    to_owner = []
    for y in range(side):
        ours = row_slots == takers[y]
        kept = jnp.where(ours[:, None, :, None], in_row, 0.0)
        to_owner.append(jnp.sum(kept, axis=(0, 2)).astype(BF16))
    at_owner = exchange(jnp.stack(to_owner), "resp", along_y)
    at_owner = jnp.sum(at_owner.astype(F32), axis=0)
    return (attended, grad_query, grad_own, jnp.swapaxes(at_owner, 0, 1)[None])


def solution(mesh):
    placed = (
        P("resp", "head"),
        P("resp", None),
        P("resp", None, None),
        P("head", None, "resp"),
        P("head", "resp", None),
        P("resp", "head"),
        P(),
        P(),
        P(),
        P(),
    )
    return jax.shard_map(
        body,
        mesh=mesh,
        in_specs=placed,
        out_specs=(
            P("resp", "head"),
            P("resp", "head"),
            P("resp", "head"),
            P("resp", None, "head"),
        ),
        check_vma=False,
    )
```

```python
import functools
import math

import jax
import jax.numpy as jnp
from jax import lax
from jax.experimental import pallas as pl
from jax.experimental.pallas import tpu as pltpu
from jax.sharding import PartitionSpec as P

F32, BF16 = jnp.float32, jnp.bfloat16
STEP_HEADS = 4
NT, TN = ((1,), (1,)), ((0,), (0,))


def dot(left, right, dims=((1,), (0,))):
    return lax.dot_general(left, right, (dims, ((), ())), preferred_element_type=F32)


def whole(*shape):
    return pl.BlockSpec(shape, lambda i, *_: (0,) * len(shape))


def keys_kernel(kp_ref, ko_ref, k_ref, kt_ref):
    parts, full, prows = kp_ref.shape
    own = ko_ref[...]
    own_rows = jnp.transpose(own)
    for r in range(parts):
        cols = kp_ref[r]
        kt_ref[r] = jnp.zeros(kt_ref.shape[1:], BF16)
        kt_ref[r, :full, :prows] = cols
        kt_ref[r, :full, prows:] = own
        k_ref[r] = jnp.zeros(k_ref.shape[1:], BF16)
        k_ref[r, :prows, :full] = jnp.transpose(cols)
        k_ref[r, prows:, :full] = own_rows


def both_keys(k_prompt, k_own):
    parts, full, prows = k_prompt.shape
    keys = prows + k_own.shape[1]
    wide = -(-full // 128) * 128
    shapes = (parts, keys, wide), (parts, wide, keys)
    return pl.pallas_call(
        keys_kernel,
        out_shape=tuple(jax.ShapeDtypeStruct(s, BF16) for s in shapes),
        grid=(1,),
        in_specs=[whole(*k_prompt.shape), whole(*k_own.shape)],
        out_specs=[whole(*s) for s in shapes],
        compiler_params=pltpu.CompilerParams(vmem_limit_bytes=12 << 20),
        name="both_keys",
    )(k_prompt, k_own)


def live_rows(rlen, parts, rows):
    spot = lax.broadcasted_iota(jnp.int32, (parts * rows, 1), 0)
    live = jnp.zeros(spot.shape, F32)
    for r in range(parts):
        alive = (spot >= r * rows) & (spot < r * rows + rlen[r])
        live = jnp.where(alive, 1.0, live)
    return live


def scores_kernel(
    sizes, plen, rlen, q_ref, ct_ref, wv_ref, wk_ref, kt_ref,
    gk_ref, w_ref, gs_ref, qf_s, gl_s, acc_s,
):
    parts, rows, heads, nope, rope, val, lat, prows = sizes
    full, width = lat + rope, nope + rope
    step = pl.program_id(0)
    scale = 1.0 / math.sqrt(width)

    @pl.when(step == 0)
    def _():
        qf_s[...] = jnp.zeros_like(qf_s)
        gl_s[...] = jnp.zeros_like(gl_s)
        acc_s[...] = jnp.zeros_like(acc_s)

    wv, wk, q, ct = wv_ref[...], wk_ref[...], q_ref[...], ct_ref[...]
    live = live_rows(rlen, parts, rows)
    for j in range(heads):
        at = j * width
        q_lat = dot(q[:, at : at + nope], wk[:, j * nope : (j + 1) * nope], NT).astype(BF16)
        q_rope = q[:, at + nope : at + width]
        heard = dot(ct[:, j * val : (j + 1) * val], wv[:, j * val : (j + 1) * val], NT)
        g_lat = (heard * live).astype(BF16)
        for r in range(parts):
            here = slice(r * rows, (r + 1) * rows)
            there = slice(j * rows, (j + 1) * rows)
            qf_s[r, there, :lat] = q_lat[here]
            qf_s[r, there, lat:full] = q_rope[here]
            gl_s[r, there, :lat] = g_lat[here]
    block, keys = heads * rows, kt_ref.shape[2]
    for r in range(parts):
        qf, gl = qf_s[r], gl_s[r]
        scores = dot(qf, kt_ref[r]) * scale
        place = lax.broadcasted_iota(jnp.int32, (block, keys), 0) % rows
        key = lax.broadcasted_iota(jnp.int32, (block, keys), 1)
        own = key - (prows + r * rows)
        valid = (key < plen[r]) | ((own >= 0) & (own <= place))
        scores = jnp.where(valid, scores, -jnp.inf)
        expo = jnp.exp(scores - jnp.max(scores, axis=1, keepdims=True))
        weights = expo / jnp.sum(expo, axis=1, keepdims=True)
        weights_bf = weights.astype(BF16)
        grad_w = dot(gl[:, :lat], kt_ref[r, :lat])
        inner = jnp.sum(weights * grad_w, axis=1, keepdims=True)
        grad_s = (weights * (grad_w - inner) * scale).astype(BF16)
        w_ref[r] = weights_bf
        gs_ref[r] = grad_s
        both = jnp.concatenate([grad_s, weights_bf], axis=0)
        rest = jnp.concatenate([qf, gl], axis=0)
        grad_k = dot(both, rest, TN)
        acc_s[r * prows : (r + 1) * prows] += grad_k[:prows]
        acc_s[parts * prows :] += grad_k[prows:]

    @pl.when(step == pl.num_programs(0) - 1)
    def _():
        gk_ref[...] = jnp.transpose(acc_s[...])[:full].astype(BF16)


def values_kernel(sizes, rlen, wv_ref, wk_ref, k_ref, w_ref, gs_ref, out_ref, gq_ref):
    parts, rows, heads, nope, rope, val, lat, prows = sizes
    full = lat + rope
    wv, wk = wv_ref[...], wk_ref[...]
    live = live_rows(rlen, parts, rows)
    lows = [dot(w_ref[r], k_ref[r, :, :lat]).astype(BF16) for r in range(parts)]
    grads = [dot(gs_ref[r], k_ref[r]).astype(BF16) for r in range(parts)]
    pieces = []
    for j in range(heads):
        there = slice(j * rows, (j + 1) * rows)
        low = jnp.concatenate([one[there] for one in lows], axis=0)
        grad = jnp.concatenate([one[there] for one in grads], axis=0)
        heard = dot(low, wv[:, j * val : (j + 1) * val]) * live
        out_ref[:, j * val : (j + 1) * val] = heard.astype(BF16)
        pieces.append(dot(grad[:, :lat], wk[:, j * nope : (j + 1) * nope]).astype(BF16))
        pieces.append(grad[:, lat:full])
    gq_ref[...] = jnp.concatenate(pieces, axis=1)


def attend(plen, rlen, queries, cotangent, weights, k, kt, full, prows, nope):
    parts, keys, wide = k.shape
    lat = weights.shape[0]
    rope = full - lat
    width = nope + rope
    tokens = queries.shape[0]
    heads = queries.shape[1] // width
    val = cotangent.shape[1] // heads
    rows = tokens // parts
    hs = STEP_HEADS
    steps = heads // hs
    sizes = (parts, rows, hs, nope, rope, val, lat, prows)
    wv_spec = pl.BlockSpec((lat, hs * val), lambda i, *_: (0, i))
    wk_spec = pl.BlockSpec((lat, hs * nope), lambda i, *_: (0, i + steps))
    q_spec = pl.BlockSpec((tokens, hs * width), lambda i, *_: (0, i))
    v_spec = pl.BlockSpec((tokens, hs * val), lambda i, *_: (0, i))
    w_spec = pl.BlockSpec((parts, hs * rows, keys), lambda i, *_: (0, i, 0))
    w_shape = jax.ShapeDtypeStruct((parts, heads * rows, keys), BF16)
    params = pltpu.CompilerParams(
        dimension_semantics=("arbitrary",), vmem_limit_bytes=30 << 20
    )
    queries, cotangent, weights, k, kt = (
        pltpu.with_memory_space_constraint(a, pltpu.HBM)
        for a in (queries, cotangent, weights, k, kt)
    )
    grad_key, soft, grad_s = pl.pallas_call(
        functools.partial(scores_kernel, sizes),
        out_shape=(
            jax.ShapeDtypeStruct((full, parts * prows + tokens), BF16),
            w_shape,
            w_shape,
        ),
        grid_spec=pltpu.PrefetchScalarGridSpec(
            num_scalar_prefetch=2,
            grid=(steps,),
            in_specs=[q_spec, v_spec, wv_spec, wk_spec, whole(*kt.shape)],
            out_specs=[whole(full, parts * prows + tokens), w_spec, w_spec],
            scratch_shapes=[
                pltpu.VMEM((parts, hs * rows, wide), BF16),
                pltpu.VMEM((parts, hs * rows, wide), BF16),
                pltpu.VMEM((parts * prows + tokens, wide), F32),
            ],
        ),
        compiler_params=params,
        cost_estimate=pl.CostEstimate(
            flops=2 * tokens * heads * (2 * lat * nope + keys * (2 * full + 2 * lat)),
            transcendentals=tokens * heads * keys,
            bytes_accessed=8 << 20,
        ),
        name="scores",
    )(plen, rlen, queries, cotangent, weights, weights, kt)
    attended, grad_query = pl.pallas_call(
        functools.partial(values_kernel, sizes),
        out_shape=(
            jax.ShapeDtypeStruct((tokens, heads * val), BF16),
            jax.ShapeDtypeStruct((tokens, heads * width), BF16),
        ),
        grid_spec=pltpu.PrefetchScalarGridSpec(
            num_scalar_prefetch=1,
            grid=(steps,),
            in_specs=[wv_spec, wk_spec, whole(*k.shape), w_spec, w_spec],
            out_specs=[v_spec, q_spec],
        ),
        compiler_params=params,
        cost_estimate=pl.CostEstimate(
            flops=2 * tokens * heads * (2 * lat * nope + keys * (full + lat)),
            transcendentals=0,
            bytes_accessed=8 << 20,
        ),
        name="values",
    )(rlen, weights, weights, k, soft, grad_s)
    return attended, grad_query, grad_key


def slots_kernel(place, in_ref, out_ref, acc_s):
    senders, _, wide = in_ref.shape
    takers, _, lanes = out_ref.shape
    parts = wide // lanes
    acc_s[...] = jnp.zeros_like(acc_s)
    for s in range(senders):
        for r in range(parts):
            to = place[s * parts + r]
            acc_s[to] += in_ref[s, :, r * lanes : (r + 1) * lanes].astype(F32)
    out_ref[...] = acc_s[:takers].astype(BF16)


def by_slot(place, in_row, takers, lanes):
    shape = (takers, in_row.shape[1], lanes)
    return pl.pallas_call(
        slots_kernel,
        out_shape=jax.ShapeDtypeStruct(shape, BF16),
        grid_spec=pltpu.PrefetchScalarGridSpec(
            num_scalar_prefetch=1,
            grid=(1,),
            in_specs=[whole(*in_row.shape)],
            out_specs=whole(*shape),
            scratch_shapes=[pltpu.VMEM((takers + 1, *shape[1:]), F32)],
        ),
        compiler_params=pltpu.CompilerParams(vmem_limit_bytes=8 << 20),
        name="by_slot",
    )(place, in_row)


def side_of(axis):
    return math.isqrt(lax.axis_size(axis))


def rows_of(side):
    return [[y * side + z for z in range(side)] for y in range(side)]


def columns_of(side):
    return [[y * side + z for y in range(side)] for z in range(side)]


def exchange(tiles, axis, groups=None):
    return lax.all_to_all(tiles, axis, 0, 0, axis_index_groups=groups, tiled=True)


def to_all(array, count, axis, groups=None):
    return exchange(jnp.broadcast_to(array, (count, *array.shape)), axis, groups)


def body(
    queries,
    resp_latent,
    prompt_latent,
    up_keys,
    up_values,
    cotangent,
    prompt_len,
    resp_len,
    resp_count,
    owner,
):
    head_devices = lax.axis_size("head")
    side = side_of("resp")
    along_z, along_y = rows_of(side), columns_of(side)
    my_index = lax.axis_index("resp")
    my_y, my_z = my_index // side, my_index % side
    head_index = lax.axis_index("head")
    heads, nope, lat_piece = up_keys.shape
    val = up_values.shape[2]
    resp_total = resp_len.shape[0]
    per_device = resp_total // lax.axis_size("resp")
    _, prompt_rows, full = prompt_latent.shape
    share = full // head_devices

    tiles = jnp.concatenate([up_values, jnp.swapaxes(up_keys, 1, 2)], axis=0)
    got = to_all(tiles, side, "resp", along_z)
    stripes = jnp.moveaxis(got, 2, 1).reshape(side * lat_piece, -1)
    weights = lax.all_gather(
        stripes, "resp", axis=0, tiled=True, axis_index_groups=along_y
    )
    cols = jnp.swapaxes(prompt_latent[0], 0, 1)
    cols = lax.dynamic_slice_in_dim(cols, head_index * share, share, 0)
    cols, _ = lax.optimization_barrier((cols, got[0, 0, 0]))
    column_prompts = to_all(cols, side, "resp", along_y)

    starts = jnp.cumsum(resp_count) - resp_count
    numbers = jnp.arange(resp_total, dtype=jnp.int32)
    prompt_of = jnp.sum((starts[None, :] <= numbers[:, None]).astype(jnp.int32), axis=1) - 1
    chosen = prompt_of[:, None] == jnp.arange(prompt_len.shape[0], dtype=jnp.int32)[None, :]
    slot_of = jnp.sum(jnp.where(chosen, owner[None, :], 0), axis=1)
    plen_of = jnp.sum(jnp.where(chosen, prompt_len[None, :], 0), axis=1)
    first = my_index * per_device
    plen_mine = lax.dynamic_slice_in_dim(plen_of, first, per_device)
    rlen_mine = lax.dynamic_slice_in_dim(resp_len, first, per_device)
    slots_mine = lax.dynamic_slice_in_dim(slot_of, first, per_device)

    by_place = slot_of.reshape(side, side, per_device)
    row_slots = lax.dynamic_index_in_dim(by_place, my_y, 0, keepdims=False)
    wanted = jnp.take(column_prompts, (row_slots // side).reshape(-1), axis=0)
    wanted = wanted.reshape(side, per_device, share, prompt_rows)
    arrived = exchange(wanted, "resp", along_z)
    mine = (slots_mine % side)[None, :] == jnp.arange(side, dtype=jnp.int32)[:, None]
    fetched = jnp.sum(
        jnp.where(mine[:, :, None, None], arrived, 0).astype(F32), axis=0
    ).astype(BF16)
    k_prompt = to_all(fetched, head_devices, "head")
    k_prompt = jnp.moveaxis(k_prompt, 0, 1).reshape(per_device, full, prompt_rows)
    k_own = jnp.swapaxes(resp_latent, 0, 1)

    k, kt = both_keys(k_prompt, k_own)

    attended, grad_query, grad_key = attend(
        plen_mine, rlen_mine, queries, cotangent, weights, k, kt, full, prompt_rows, nope
    )
    by_head = exchange(grad_key.reshape(head_devices, share, -1), "head")
    summed = jnp.sum(by_head.astype(F32), axis=0)
    split = per_device * prompt_rows
    grad_own = jnp.swapaxes(summed[:, split:], 0, 1)
    grad_prompt = summed[:, :split].astype(BF16)
    in_row = to_all(grad_prompt, side, "resp", along_z)
    place = jnp.where(row_slots % side == my_z, row_slots // side, side).reshape(-1)
    to_owner = by_slot(place, in_row, side, prompt_rows)
    at_owner = exchange(to_owner, "resp", along_y)
    at_owner = jnp.sum(at_owner.astype(F32), axis=0)
    return (attended, grad_query, grad_own, jnp.swapaxes(at_owner, 0, 1)[None])


def solution(mesh):
    placed = (
        P("resp", "head"),
        P("resp", None),
        P("resp", None, None),
        P("head", None, "resp"),
        P("head", "resp", None),
        P("resp", "head"),
        P(),
        P(),
        P(),
        P(),
    )
    return jax.shard_map(
        body,
        mesh=mesh,
        in_specs=placed,
        out_specs=(
            P("resp", "head"),
            P("resp", "head"),
            P("resp", "head"),
            P("resp", None, "head"),
        ),
        check_vma=False,
    )
```

```python
import functools
import math

import jax
import jax.numpy as jnp
from jax import lax
from jax.experimental import pallas as pl
from jax.experimental.pallas import tpu as pltpu
from jax.sharding import PartitionSpec as P

F32, BF16 = jnp.float32, jnp.bfloat16
SCORE_HEADS, VALUE_HEADS = 16, 8
NT, TN = ((1,), (1,)), ((0,), (0,))


def dot(left, right, dims=((1,), (0,))):
    return lax.dot_general(left, right, (dims, ((), ())), preferred_element_type=F32)


def whole(*shape):
    return pl.BlockSpec(shape, lambda i, *_: (0,) * len(shape))


def keys_kernel(kp_ref, ko_ref, k_ref, kt_ref):
    parts, full, prows = kp_ref.shape
    own = ko_ref[...]
    own_rows = jnp.transpose(own)
    for r in range(parts):
        cols = kp_ref[r]
        kt_ref[r] = jnp.zeros(kt_ref.shape[1:], BF16)
        kt_ref[r, :full, :prows] = cols
        kt_ref[r, :full, prows:] = own
        k_ref[r] = jnp.zeros(k_ref.shape[1:], BF16)
        k_ref[r, :prows, :full] = jnp.transpose(cols)
        k_ref[r, prows:, :full] = own_rows


def both_keys(k_prompt, k_own):
    parts, full, prows = k_prompt.shape
    keys = prows + k_own.shape[1]
    wide = -(-full // 128) * 128
    shapes = (parts, keys, wide), (parts, wide, keys)
    return pl.pallas_call(
        keys_kernel,
        out_shape=tuple(jax.ShapeDtypeStruct(s, BF16) for s in shapes),
        grid=(1,),
        in_specs=[whole(*k_prompt.shape), whole(*k_own.shape)],
        out_specs=[whole(*s) for s in shapes],
        compiler_params=pltpu.CompilerParams(vmem_limit_bytes=12 << 20),
        name="both_keys",
    )(k_prompt, k_own)


def live_rows(rlen, parts, rows):
    spot = lax.broadcasted_iota(jnp.int32, (parts * rows, 1), 0)
    live = jnp.zeros(spot.shape, F32)
    for r in range(parts):
        alive = (spot >= r * rows) & (spot < r * rows + rlen[r])
        live = jnp.where(alive, 1.0, live)
    return live


def scores_kernel(
    sizes, plen, rlen, q_ref, ct_ref, wv_ref, wk_ref, kt_ref,
    gk_ref, w_ref, gs_ref, qf_s, gl_s, acc_s, bias_s,
):
    parts, rows, heads, nope, rope, val, lat, prows = sizes
    full, width = lat + rope, nope + rope
    step = pl.program_id(0)
    scale = 1.0 / math.sqrt(width)

    @pl.when(step == 0)
    def _():
        qf_s[...] = jnp.zeros_like(qf_s)
        gl_s[...] = jnp.zeros_like(gl_s)
        acc_s[...] = jnp.zeros_like(acc_s)
        for r in range(parts):
            place = lax.broadcasted_iota(jnp.int32, bias_s.shape[1:], 0) % rows
            key = lax.broadcasted_iota(jnp.int32, bias_s.shape[1:], 1)
            own = key - (prows + r * rows)
            valid = (key < plen[r]) | ((own >= 0) & (own <= place))
            bias_s[r] = jnp.where(valid, 0.0, -jnp.inf)

    wv, wk, q, ct = wv_ref[...], wk_ref[...], q_ref[...], ct_ref[...]
    live = live_rows(rlen, parts, rows)
    for j in range(heads):
        at = j * width
        q_lat = dot(q[:, at : at + nope], wk[:, j * nope : (j + 1) * nope], NT).astype(BF16)
        q_rope = q[:, at + nope : at + width]
        heard = dot(ct[:, j * val : (j + 1) * val], wv[:, j * val : (j + 1) * val], NT)
        g_lat = (heard * live).astype(BF16)
        for r in range(parts):
            here = slice(r * rows, (r + 1) * rows)
            there = slice(j * rows, (j + 1) * rows)
            qf_s[r, there, :lat] = q_lat[here]
            qf_s[r, there, lat:full] = q_rope[here]
            gl_s[r, there, :lat] = g_lat[here]
    raw = [dot(qf_s[r], kt_ref[r]) for r in range(parts)]
    heard = [dot(gl_s[r, :, :lat], kt_ref[r, :lat]) for r in range(parts)]
    for r in range(parts):
        scores = raw[r] * scale + bias_s[r]
        expo = jnp.exp(scores - jnp.max(scores, axis=1, keepdims=True))
        weights = expo * (1.0 / jnp.sum(expo, axis=1, keepdims=True))
        inner = jnp.sum(weights * heard[r], axis=1, keepdims=True)
        w_ref[r] = weights.astype(BF16)
        gs_ref[r] = (weights * (heard[r] - inner) * scale).astype(BF16)
    for r in range(parts):
        grad_k = dot(gs_ref[r], qf_s[r], TN)
        grad_v = dot(w_ref[r], gl_s[r, :, :lat], TN)
        at = slice(r * prows, (r + 1) * prows)
        acc_s[at] += grad_k[:prows]
        acc_s[parts * prows :] += grad_k[prows:]
        acc_s[at, :lat] += grad_v[:prows]
        acc_s[parts * prows :, :lat] += grad_v[prows:]

    @pl.when(step == pl.num_programs(0) - 1)
    def _():
        gk_ref[...] = jnp.transpose(acc_s[...])[:full].astype(BF16)


def values_kernel(sizes, rlen, wv_ref, wk_ref, k_ref, w_ref, gs_ref, out_ref, gq_ref):
    parts, rows, heads, nope, rope, val, lat, prows = sizes
    full = lat + rope
    wv, wk = wv_ref[...], wk_ref[...]
    live = live_rows(rlen, parts, rows)
    lows = [dot(w_ref[r], k_ref[r, :, :lat]).astype(BF16) for r in range(parts)]
    grads = [dot(gs_ref[r], k_ref[r]).astype(BF16) for r in range(parts)]
    pieces = []
    for j in range(heads):
        there = slice(j * rows, (j + 1) * rows)
        low = jnp.concatenate([one[there] for one in lows], axis=0)
        grad = jnp.concatenate([one[there] for one in grads], axis=0)
        heard = dot(low, wv[:, j * val : (j + 1) * val]) * live
        out_ref[:, j * val : (j + 1) * val] = heard.astype(BF16)
        pieces.append(dot(grad[:, :lat], wk[:, j * nope : (j + 1) * nope]).astype(BF16))
        pieces.append(grad[:, lat:full])
    gq_ref[...] = jnp.concatenate(pieces, axis=1)


def attend(plen, rlen, queries, cotangent, weights, k, kt, full, prows, nope):
    parts, keys, wide = k.shape
    lat = weights.shape[0]
    rope = full - lat
    width = nope + rope
    tokens = queries.shape[0]
    heads = queries.shape[1] // width
    val = cotangent.shape[1] // heads
    rows = tokens // parts
    hs, vs = SCORE_HEADS, VALUE_HEADS
    sizes = (parts, rows, hs, nope, rope, val, lat, prows)
    w_shape = jax.ShapeDtypeStruct((parts, heads * rows, keys), BF16)

    def specs(count):
        steps = heads // count
        return (
            pl.BlockSpec((lat, count * val), lambda i, *_: (0, i)),
            pl.BlockSpec((lat, count * nope), lambda i, *_: (0, i + steps)),
            pl.BlockSpec((tokens, count * width), lambda i, *_: (0, i)),
            pl.BlockSpec((tokens, count * val), lambda i, *_: (0, i)),
            pl.BlockSpec((parts, count * rows, keys), lambda i, *_: (0, i, 0)),
        )

    wv_spec, wk_spec, q_spec, v_spec, w_spec = specs(hs)
    params = pltpu.CompilerParams(
        dimension_semantics=("arbitrary",), vmem_limit_bytes=30 << 20
    )
    queries, cotangent, weights, k, kt = (
        pltpu.with_memory_space_constraint(a, pltpu.HBM)
        for a in (queries, cotangent, weights, k, kt)
    )
    grad_key, soft, grad_s = pl.pallas_call(
        functools.partial(scores_kernel, sizes),
        out_shape=(
            jax.ShapeDtypeStruct((full, parts * prows + tokens), BF16),
            w_shape,
            w_shape,
        ),
        grid_spec=pltpu.PrefetchScalarGridSpec(
            num_scalar_prefetch=2,
            grid=(heads // hs,),
            in_specs=[q_spec, v_spec, wv_spec, wk_spec, whole(*kt.shape)],
            out_specs=[whole(full, parts * prows + tokens), w_spec, w_spec],
            scratch_shapes=[
                pltpu.VMEM((parts, hs * rows, wide), BF16),
                pltpu.VMEM((parts, hs * rows, wide), BF16),
                pltpu.VMEM((parts * prows + tokens, wide), F32),
                pltpu.VMEM((parts, hs * rows, keys), F32),
            ],
        ),
        compiler_params=params,
        cost_estimate=pl.CostEstimate(
            flops=2 * tokens * heads * (2 * lat * nope + keys * (2 * full + 2 * lat)),
            transcendentals=tokens * heads * keys,
            bytes_accessed=8 << 20,
        ),
        name="scores",
    )(plen, rlen, queries, cotangent, weights, weights, kt)
    wv_spec, wk_spec, q_spec, v_spec, w_spec = specs(vs)
    sizes = (parts, rows, vs, nope, rope, val, lat, prows)
    attended, grad_query = pl.pallas_call(
        functools.partial(values_kernel, sizes),
        out_shape=(
            jax.ShapeDtypeStruct((tokens, heads * val), BF16),
            jax.ShapeDtypeStruct((tokens, heads * width), BF16),
        ),
        grid_spec=pltpu.PrefetchScalarGridSpec(
            num_scalar_prefetch=1,
            grid=(heads // vs,),
            in_specs=[wv_spec, wk_spec, whole(*k.shape), w_spec, w_spec],
            out_specs=[v_spec, q_spec],
        ),
        compiler_params=params,
        cost_estimate=pl.CostEstimate(
            flops=2 * tokens * heads * (2 * lat * nope + keys * (full + lat)),
            transcendentals=0,
            bytes_accessed=8 << 20,
        ),
        name="values",
    )(rlen, weights, weights, k, soft, grad_s)
    return attended, grad_query, grad_key


def slots_kernel(place, in_ref, out_ref, acc_s):
    senders, _, wide = in_ref.shape
    takers, _, lanes = out_ref.shape
    parts = wide // lanes
    acc_s[...] = jnp.zeros_like(acc_s)
    for s in range(senders):
        for r in range(parts):
            to = place[s * parts + r]
            acc_s[to] += in_ref[s, :, r * lanes : (r + 1) * lanes].astype(F32)
    out_ref[...] = acc_s[:takers].astype(BF16)


def by_slot(place, in_row, takers, lanes):
    shape = (takers, in_row.shape[1], lanes)
    return pl.pallas_call(
        slots_kernel,
        out_shape=jax.ShapeDtypeStruct(shape, BF16),
        grid_spec=pltpu.PrefetchScalarGridSpec(
            num_scalar_prefetch=1,
            grid=(1,),
            in_specs=[whole(*in_row.shape)],
            out_specs=whole(*shape),
            scratch_shapes=[pltpu.VMEM((takers + 1, *shape[1:]), F32)],
        ),
        compiler_params=pltpu.CompilerParams(vmem_limit_bytes=8 << 20),
        name="by_slot",
    )(place, in_row)


def side_of(axis):
    return math.isqrt(lax.axis_size(axis))


def rows_of(side):
    return [[y * side + z for z in range(side)] for y in range(side)]


def columns_of(side):
    return [[y * side + z for y in range(side)] for z in range(side)]


def exchange(tiles, axis, groups=None):
    return lax.all_to_all(tiles, axis, 0, 0, axis_index_groups=groups, tiled=True)


def to_all(array, count, axis, groups=None):
    return exchange(jnp.broadcast_to(array, (count, *array.shape)), axis, groups)


def body(
    queries,
    resp_latent,
    prompt_latent,
    up_keys,
    up_values,
    cotangent,
    prompt_len,
    resp_len,
    resp_count,
    owner,
):
    head_devices = lax.axis_size("head")
    side = side_of("resp")
    along_z, along_y = rows_of(side), columns_of(side)
    my_index = lax.axis_index("resp")
    my_y, my_z = my_index // side, my_index % side
    head_index = lax.axis_index("head")
    heads, nope, lat_piece = up_keys.shape
    val = up_values.shape[2]
    resp_total = resp_len.shape[0]
    per_device = resp_total // lax.axis_size("resp")
    _, prompt_rows, full = prompt_latent.shape
    share = full // head_devices

    tiles = jnp.concatenate([up_values, jnp.swapaxes(up_keys, 1, 2)], axis=0)
    got = to_all(tiles, side, "resp", along_z)
    stripes = jnp.moveaxis(got, 2, 1).reshape(side * lat_piece, -1)
    weights = lax.all_gather(
        stripes, "resp", axis=0, tiled=True, axis_index_groups=along_y
    )
    cols = jnp.swapaxes(prompt_latent[0], 0, 1)
    cols = lax.dynamic_slice_in_dim(cols, head_index * share, share, 0)
    cols, _ = lax.optimization_barrier((cols, got[0, 0, 0]))
    column_prompts = to_all(cols, side, "resp", along_y)

    starts = jnp.cumsum(resp_count) - resp_count
    numbers = jnp.arange(resp_total, dtype=jnp.int32)
    prompt_of = jnp.sum((starts[None, :] <= numbers[:, None]).astype(jnp.int32), axis=1) - 1
    chosen = prompt_of[:, None] == jnp.arange(prompt_len.shape[0], dtype=jnp.int32)[None, :]
    slot_of = jnp.sum(jnp.where(chosen, owner[None, :], 0), axis=1)
    plen_of = jnp.sum(jnp.where(chosen, prompt_len[None, :], 0), axis=1)
    first = my_index * per_device
    plen_mine = lax.dynamic_slice_in_dim(plen_of, first, per_device)
    rlen_mine = lax.dynamic_slice_in_dim(resp_len, first, per_device)
    slots_mine = lax.dynamic_slice_in_dim(slot_of, first, per_device)

    by_place = slot_of.reshape(side, side, per_device)
    row_slots = lax.dynamic_index_in_dim(by_place, my_y, 0, keepdims=False)
    wanted = jnp.take(column_prompts, (row_slots // side).reshape(-1), axis=0)
    wanted = wanted.reshape(side, per_device, share, prompt_rows)
    arrived = exchange(wanted, "resp", along_z)
    mine = (slots_mine % side)[None, :] == jnp.arange(side, dtype=jnp.int32)[:, None]
    fetched = jnp.sum(
        jnp.where(mine[:, :, None, None], arrived, 0).astype(F32), axis=0
    ).astype(BF16)
    k_prompt = to_all(fetched, head_devices, "head")
    k_prompt = jnp.moveaxis(k_prompt, 0, 1).reshape(per_device, full, prompt_rows)
    k_own = jnp.swapaxes(resp_latent, 0, 1)

    k, kt = both_keys(k_prompt, k_own)

    attended, grad_query, grad_key = attend(
        plen_mine, rlen_mine, queries, cotangent, weights, k, kt, full, prompt_rows, nope
    )
    by_head = exchange(grad_key.reshape(head_devices, share, -1), "head")
    summed = jnp.sum(by_head.astype(F32), axis=0)
    split = per_device * prompt_rows
    grad_own = jnp.swapaxes(summed[:, split:], 0, 1)
    grad_prompt = summed[:, :split].astype(BF16)
    in_row = to_all(grad_prompt, side, "resp", along_z)
    place = jnp.where(row_slots % side == my_z, row_slots // side, side).reshape(-1)
    place, attended = lax.optimization_barrier((place, attended))
    to_owner = by_slot(place, in_row, side, prompt_rows)
    at_owner = exchange(to_owner, "resp", along_y)
    at_owner = jnp.sum(at_owner.astype(F32), axis=0)
    return (attended, grad_query, grad_own, jnp.swapaxes(at_owner, 0, 1)[None])


def solution(mesh):
    placed = (
        P("resp", "head"),
        P("resp", None),
        P("resp", None, None),
        P("head", None, "resp"),
        P("head", "resp", None),
        P("resp", "head"),
        P(),
        P(),
        P(),
        P(),
    )
    return jax.shard_map(
        body,
        mesh=mesh,
        in_specs=placed,
        out_specs=(
            P("resp", "head"),
            P("resp", "head"),
            P("resp", "head"),
            P("resp", None, "head"),
        ),
        check_vma=False,
    )
```

```python
import functools
import math

import jax
import jax.numpy as jnp
from jax import lax
from jax.experimental import pallas as pl
from jax.experimental.pallas import tpu as pltpu
from jax.sharding import PartitionSpec as P

F32, BF16 = jnp.float32, jnp.bfloat16
SCORE_HEADS, VALUE_HEADS = 16, 8
NT, TN = ((1,), (1,)), ((0,), (0,))


def dot(left, right, dims=((1,), (0,))):
    return lax.dot_general(left, right, (dims, ((), ())), preferred_element_type=F32)


def whole(*shape):
    return pl.BlockSpec(shape, lambda i, *_: (0,) * len(shape))


def keys_kernel(kp_ref, ko_ref, k_ref, kt_ref):
    parts, full, prows = kp_ref.shape
    own = ko_ref[...]
    own_rows = jnp.transpose(own)
    for r in range(parts):
        cols = kp_ref[r]
        kt_ref[r] = jnp.zeros(kt_ref.shape[1:], BF16)
        kt_ref[r, :full, :prows] = cols
        kt_ref[r, :full, prows:] = own
        k_ref[r] = jnp.zeros(k_ref.shape[1:], BF16)
        k_ref[r, :prows, :full] = jnp.transpose(cols)
        k_ref[r, prows:, :full] = own_rows


def both_keys(k_prompt, k_own):
    parts, full, prows = k_prompt.shape
    keys = prows + k_own.shape[1]
    wide = -(-full // 128) * 128
    shapes = (parts, keys, wide), (parts, wide, keys)
    return pl.pallas_call(
        keys_kernel,
        out_shape=tuple(jax.ShapeDtypeStruct(s, BF16) for s in shapes),
        grid=(1,),
        in_specs=[whole(*k_prompt.shape), whole(*k_own.shape)],
        out_specs=[whole(*s) for s in shapes],
        compiler_params=pltpu.CompilerParams(vmem_limit_bytes=12 << 20),
        name="both_keys",
    )(k_prompt, k_own)


def live_rows(rlen, parts, rows):
    spot = lax.broadcasted_iota(jnp.int32, (parts * rows, 1), 0)
    live = jnp.zeros(spot.shape, F32)
    for r in range(parts):
        alive = (spot >= r * rows) & (spot < r * rows + rlen[r])
        live = jnp.where(alive, 1.0, live)
    return live


def scores_kernel(
    sizes, plen, rlen, q_ref, ct_ref, wv_ref, wk_ref, kt_ref,
    gk_ref, go_ref, w_ref, gs_ref, qf_s, gl_s, acc_s, bias_s,
):
    parts, rows, heads, nope, rope, val, lat, prows = sizes
    full, width = lat + rope, nope + rope
    step = pl.program_id(0)
    scale = 1.0 / math.sqrt(width)

    @pl.when(step == 0)
    def _():
        qf_s[...] = jnp.zeros_like(qf_s)
        gl_s[...] = jnp.zeros_like(gl_s)
        acc_s[...] = jnp.zeros_like(acc_s)
        for r in range(parts):
            place = lax.broadcasted_iota(jnp.int32, bias_s.shape[1:], 0) % rows
            key = lax.broadcasted_iota(jnp.int32, bias_s.shape[1:], 1)
            own = key - (prows + r * rows)
            valid = (key < plen[r]) | ((own >= 0) & (own <= place))
            bias_s[r] = jnp.where(valid, 0.0, -jnp.inf)

    wv, wk, q, ct = wv_ref[...], wk_ref[...], q_ref[...], ct_ref[...]
    live = live_rows(rlen, parts, rows)
    for j in range(heads):
        at = j * width
        q_lat = dot(q[:, at : at + nope], wk[:, j * nope : (j + 1) * nope], NT).astype(BF16)
        q_rope = q[:, at + nope : at + width]
        heard = dot(ct[:, j * val : (j + 1) * val], wv[:, j * val : (j + 1) * val], NT)
        g_lat = (heard * live).astype(BF16)
        for r in range(parts):
            here = slice(r * rows, (r + 1) * rows)
            there = slice(j * rows, (j + 1) * rows)
            qf_s[r, there, :lat] = q_lat[here]
            qf_s[r, there, lat:full] = q_rope[here]
            gl_s[r, there, :lat] = g_lat[here]
    raw = [dot(qf_s[r], kt_ref[r]) for r in range(parts)]
    heard = [dot(gl_s[r, :, :lat], kt_ref[r, :lat]) for r in range(parts)]
    for r in range(parts):
        scores = raw[r] * scale + bias_s[r]
        expo = jnp.exp(scores - jnp.max(scores, axis=1, keepdims=True))
        weights = expo * (1.0 / jnp.sum(expo, axis=1, keepdims=True))
        inner = jnp.sum(weights * heard[r], axis=1, keepdims=True)
        w_ref[r] = weights.astype(BF16)
        gs_ref[r] = (weights * (heard[r] - inner) * scale).astype(BF16)
    for r in range(parts):
        grad_k = dot(gs_ref[r], qf_s[r], TN)
        grad_v = dot(w_ref[r], gl_s[r, :, :lat], TN)
        at = slice(r * prows, (r + 1) * prows)
        acc_s[at] += grad_k[:prows]
        acc_s[parts * prows :] += grad_k[prows:]
        acc_s[at, :lat] += grad_v[:prows]
        acc_s[parts * prows :, :lat] += grad_v[prows:]

    @pl.when(step == pl.num_programs(0) - 1)
    def _():
        turned = jnp.transpose(acc_s[...])[:full]
        gk_ref[...] = turned[:, : parts * prows].astype(BF16)
        go_ref[...] = turned[:, parts * prows :]


def values_kernel(sizes, rlen, wv_ref, wk_ref, k_ref, w_ref, gs_ref, out_ref, gq_ref):
    parts, rows, heads, nope, rope, val, lat, prows = sizes
    full = lat + rope
    wv, wk = wv_ref[...], wk_ref[...]
    live = live_rows(rlen, parts, rows)
    lows = [dot(w_ref[r], k_ref[r, :, :lat]).astype(BF16) for r in range(parts)]
    grads = [dot(gs_ref[r], k_ref[r]).astype(BF16) for r in range(parts)]
    pieces = []
    for j in range(heads):
        there = slice(j * rows, (j + 1) * rows)
        low = jnp.concatenate([one[there] for one in lows], axis=0)
        grad = jnp.concatenate([one[there] for one in grads], axis=0)
        heard = dot(low, wv[:, j * val : (j + 1) * val]) * live
        out_ref[:, j * val : (j + 1) * val] = heard.astype(BF16)
        pieces.append(dot(grad[:, :lat], wk[:, j * nope : (j + 1) * nope]).astype(BF16))
        pieces.append(grad[:, lat:full])
    gq_ref[...] = jnp.concatenate(pieces, axis=1)


def attend(plen, rlen, queries, cotangent, weights, k, kt, full, prows, nope):
    parts, keys, wide = k.shape
    lat = weights.shape[0]
    rope = full - lat
    width = nope + rope
    tokens = queries.shape[0]
    heads = queries.shape[1] // width
    val = cotangent.shape[1] // heads
    rows = tokens // parts
    hs, vs = SCORE_HEADS, VALUE_HEADS
    sizes = (parts, rows, hs, nope, rope, val, lat, prows)
    w_shape = jax.ShapeDtypeStruct((parts, heads * rows, keys), BF16)

    def specs(count):
        steps = heads // count
        return (
            pl.BlockSpec((lat, count * val), lambda i, *_: (0, i)),
            pl.BlockSpec((lat, count * nope), lambda i, *_: (0, i + steps)),
            pl.BlockSpec((tokens, count * width), lambda i, *_: (0, i)),
            pl.BlockSpec((tokens, count * val), lambda i, *_: (0, i)),
            pl.BlockSpec((parts, count * rows, keys), lambda i, *_: (0, i, 0)),
        )

    wv_spec, wk_spec, q_spec, v_spec, w_spec = specs(hs)
    params = pltpu.CompilerParams(
        dimension_semantics=("arbitrary",), vmem_limit_bytes=30 << 20
    )
    queries, cotangent, weights, k, kt = (
        pltpu.with_memory_space_constraint(a, pltpu.HBM)
        for a in (queries, cotangent, weights, k, kt)
    )
    grad_key, grad_own, soft, grad_s = pl.pallas_call(
        functools.partial(scores_kernel, sizes),
        out_shape=(
            jax.ShapeDtypeStruct((full, parts * prows), BF16),
            jax.ShapeDtypeStruct((full, tokens), F32),
            w_shape,
            w_shape,
        ),
        grid_spec=pltpu.PrefetchScalarGridSpec(
            num_scalar_prefetch=2,
            grid=(heads // hs,),
            in_specs=[q_spec, v_spec, wv_spec, wk_spec, whole(*kt.shape)],
            out_specs=[whole(full, parts * prows), whole(full, tokens), w_spec, w_spec],
            scratch_shapes=[
                pltpu.VMEM((parts, hs * rows, wide), BF16),
                pltpu.VMEM((parts, hs * rows, wide), BF16),
                pltpu.VMEM((parts * prows + tokens, wide), F32),
                pltpu.VMEM((parts, hs * rows, keys), F32),
            ],
        ),
        compiler_params=params,
        cost_estimate=pl.CostEstimate(
            flops=2 * tokens * heads * (2 * lat * nope + keys * (2 * full + 2 * lat)),
            transcendentals=tokens * heads * keys,
            bytes_accessed=8 << 20,
        ),
        name="scores",
    )(plen, rlen, queries, cotangent, weights, weights, kt)
    wv_spec, wk_spec, q_spec, v_spec, w_spec = specs(vs)
    sizes = (parts, rows, vs, nope, rope, val, lat, prows)
    attended, grad_query = pl.pallas_call(
        functools.partial(values_kernel, sizes),
        out_shape=(
            jax.ShapeDtypeStruct((tokens, heads * val), BF16),
            jax.ShapeDtypeStruct((tokens, heads * width), BF16),
        ),
        grid_spec=pltpu.PrefetchScalarGridSpec(
            num_scalar_prefetch=1,
            grid=(heads // vs,),
            in_specs=[wv_spec, wk_spec, whole(*k.shape), w_spec, w_spec],
            out_specs=[v_spec, q_spec],
        ),
        compiler_params=params,
        cost_estimate=pl.CostEstimate(
            flops=2 * tokens * heads * (2 * lat * nope + keys * (full + lat)),
            transcendentals=0,
            bytes_accessed=8 << 20,
        ),
        name="values",
    )(rlen, weights, weights, k, soft, grad_s)
    return attended, grad_query, grad_key, grad_own


def slots_kernel(place, in_ref, out_ref, acc_s):
    senders, _, wide = in_ref.shape
    takers, _, lanes = out_ref.shape
    parts = wide // lanes
    acc_s[...] = jnp.zeros_like(acc_s)
    for s in range(senders):
        for r in range(parts):
            to = place[s * parts + r]
            acc_s[to] += in_ref[s, :, r * lanes : (r + 1) * lanes].astype(F32)
    out_ref[...] = acc_s[:takers].astype(BF16)


def by_slot(place, in_row, takers, lanes):
    shape = (takers, in_row.shape[1], lanes)
    return pl.pallas_call(
        slots_kernel,
        out_shape=jax.ShapeDtypeStruct(shape, BF16),
        grid_spec=pltpu.PrefetchScalarGridSpec(
            num_scalar_prefetch=1,
            grid=(1,),
            in_specs=[whole(*in_row.shape)],
            out_specs=whole(*shape),
            scratch_shapes=[pltpu.VMEM((takers + 1, *shape[1:]), F32)],
        ),
        compiler_params=pltpu.CompilerParams(vmem_limit_bytes=8 << 20),
        name="by_slot",
    )(place, in_row)


def side_of(axis):
    return math.isqrt(lax.axis_size(axis))


def rows_of(side):
    return [[y * side + z for z in range(side)] for y in range(side)]


def columns_of(side):
    return [[y * side + z for y in range(side)] for z in range(side)]


def exchange(tiles, axis, groups=None):
    return lax.all_to_all(tiles, axis, 0, 0, axis_index_groups=groups, tiled=True)


def to_all(array, count, axis, groups=None):
    return exchange(jnp.broadcast_to(array, (count, *array.shape)), axis, groups)


def body(
    queries,
    resp_latent,
    prompt_latent,
    up_keys,
    up_values,
    cotangent,
    prompt_len,
    resp_len,
    resp_count,
    owner,
):
    head_devices = lax.axis_size("head")
    side = side_of("resp")
    along_z, along_y = rows_of(side), columns_of(side)
    my_index = lax.axis_index("resp")
    my_y, my_z = my_index // side, my_index % side
    head_index = lax.axis_index("head")
    heads, nope, lat_piece = up_keys.shape
    val = up_values.shape[2]
    resp_total = resp_len.shape[0]
    per_device = resp_total // lax.axis_size("resp")
    _, prompt_rows, full = prompt_latent.shape
    share = full // head_devices

    tiles = jnp.concatenate([up_values, jnp.swapaxes(up_keys, 1, 2)], axis=0)
    got = to_all(tiles, side, "resp", along_z)
    stripes = jnp.moveaxis(got, 2, 1).reshape(side * lat_piece, -1)
    weights = lax.all_gather(
        stripes, "resp", axis=0, tiled=True, axis_index_groups=along_y
    )
    cols = jnp.swapaxes(prompt_latent[0], 0, 1)
    cols = lax.dynamic_slice_in_dim(cols, head_index * share, share, 0)
    cols, _ = lax.optimization_barrier((cols, got[0, 0, 0]))
    column_prompts = to_all(cols, side, "resp", along_y)

    starts = jnp.cumsum(resp_count) - resp_count
    numbers = jnp.arange(resp_total, dtype=jnp.int32)
    prompt_of = jnp.sum((starts[None, :] <= numbers[:, None]).astype(jnp.int32), axis=1) - 1
    chosen = prompt_of[:, None] == jnp.arange(prompt_len.shape[0], dtype=jnp.int32)[None, :]
    slot_of = jnp.sum(jnp.where(chosen, owner[None, :], 0), axis=1)
    plen_of = jnp.sum(jnp.where(chosen, prompt_len[None, :], 0), axis=1)
    first = my_index * per_device
    plen_mine = lax.dynamic_slice_in_dim(plen_of, first, per_device)
    rlen_mine = lax.dynamic_slice_in_dim(resp_len, first, per_device)
    slots_mine = lax.dynamic_slice_in_dim(slot_of, first, per_device)

    by_place = slot_of.reshape(side, side, per_device)
    row_slots = lax.dynamic_index_in_dim(by_place, my_y, 0, keepdims=False)
    wanted = jnp.take(column_prompts, (row_slots // side).reshape(-1), axis=0)
    wanted = wanted.reshape(side, per_device, share, prompt_rows)
    arrived = exchange(wanted, "resp", along_z)
    mine = (slots_mine % side)[None, :] == jnp.arange(side, dtype=jnp.int32)[:, None]
    fetched = jnp.sum(
        jnp.where(mine[:, :, None, None], arrived, 0).astype(F32), axis=0
    ).astype(BF16)
    k_prompt = to_all(fetched, head_devices, "head")
    k_prompt = jnp.moveaxis(k_prompt, 0, 1).reshape(per_device, full, prompt_rows)
    k_own = jnp.swapaxes(resp_latent, 0, 1)

    place = jnp.where(row_slots % side == my_z, row_slots // side, side).reshape(-1)
    k_prompt, place = lax.optimization_barrier((k_prompt, place))
    k, kt = both_keys(k_prompt, k_own)

    attended, grad_query, grad_key, grad_own = attend(
        plen_mine, rlen_mine, queries, cotangent, weights, k, kt, full, prompt_rows, nope
    )
    grad_own = lax.psum_scatter(grad_own, "head", scatter_dimension=0, tiled=True)
    grad_own = jnp.swapaxes(grad_own, 0, 1)
    by_head = exchange(grad_key.reshape(head_devices, share, -1), "head")
    grad_prompt = jnp.sum(by_head.astype(F32), axis=0).astype(BF16)
    grad_prompt, attended = lax.optimization_barrier((grad_prompt, attended))
    in_row = to_all(grad_prompt, side, "resp", along_z)
    to_owner = by_slot(place, in_row, side, prompt_rows)
    at_owner = exchange(to_owner, "resp", along_y)
    at_owner = jnp.sum(at_owner.astype(F32), axis=0)
    return (attended, grad_query, grad_own, jnp.swapaxes(at_owner, 0, 1)[None])


def solution(mesh):
    placed = (
        P("resp", "head"),
        P("resp", None),
        P("resp", None, None),
        P("head", None, "resp"),
        P("head", "resp", None),
        P("resp", "head"),
        P(),
        P(),
        P(),
        P(),
    )
    return jax.shard_map(
        body,
        mesh=mesh,
        in_specs=placed,
        out_specs=(
            P("resp", "head"),
            P("resp", "head"),
            P("resp", "head"),
            P("resp", None, "head"),
        ),
        check_vma=False,
    )
```

```python
import functools
import math

import jax
import jax.numpy as jnp
from jax import lax
from jax.experimental import pallas as pl
from jax.experimental.pallas import tpu as pltpu
from jax.sharding import PartitionSpec as P

F32, BF16 = jnp.float32, jnp.bfloat16
CHUNKS, VALUE_HEADS = 4, 8
NT, TN = ((1,), (1,)), ((0,), (0,))


def dot(left, right, dims=((1,), (0,))):
    return lax.dot_general(left, right, (dims, ((), ())), preferred_element_type=F32)


def whole(*shape):
    return pl.BlockSpec(shape, lambda i, *_: (0,) * len(shape))


def keys_kernel(kp_ref, ko_ref, k_ref, kt_ref):
    parts, full, prows = kp_ref.shape
    own = ko_ref[...]
    own_rows = jnp.transpose(own)
    for r in range(parts):
        cols = kp_ref[r]
        kt_ref[r] = jnp.zeros(kt_ref.shape[1:], BF16)
        kt_ref[r, :full, :prows] = cols
        kt_ref[r, :full, prows:] = own
        k_ref[r] = jnp.zeros(k_ref.shape[1:], BF16)
        k_ref[r, :prows, :full] = jnp.transpose(cols)
        k_ref[r, prows:, :full] = own_rows


def both_keys(k_prompt, k_own):
    parts, full, prows = k_prompt.shape
    keys = prows + k_own.shape[1]
    wide = -(-full // 128) * 128
    shapes = (parts, keys, wide), (parts, wide, keys)
    return pl.pallas_call(
        keys_kernel,
        out_shape=tuple(jax.ShapeDtypeStruct(s, BF16) for s in shapes),
        grid=(1,),
        in_specs=[whole(*k_prompt.shape), whole(*k_own.shape)],
        out_specs=[whole(*s) for s in shapes],
        compiler_params=pltpu.CompilerParams(vmem_limit_bytes=12 << 20),
        name="both_keys",
    )(k_prompt, k_own)


def live_rows(rlen, parts, rows):
    spot = lax.broadcasted_iota(jnp.int32, (parts * rows, 1), 0)
    live = jnp.zeros(spot.shape, F32)
    for r in range(parts):
        alive = (spot >= r * rows) & (spot < r * rows + rlen[r])
        live = jnp.where(alive, 1.0, live)
    return live


def scores_kernel(
    sizes, plen, rlen, q_hbm, ct_hbm, w_hbm, kt_hbm,
    gk_ref, go_ref, w_ref, gs_ref,
    q_s, ct_s, wv_s, wk_s, kt_s, qf_s, gl_s, sems,
):
    parts, rows, heads, nope, rope, val, lat, prows = sizes
    full, width = lat + rope, nope + rope
    scale = 1.0 / math.sqrt(width)
    chunk = heads // CHUNKS
    copies = []
    for c in range(CHUNKS):
        for t, (source, target, size, first) in enumerate((
            (w_hbm, wk_s, chunk * nope, heads * val),
            (q_hbm, q_s, chunk * width, 0),
            (w_hbm, wv_s, chunk * val, 0),
            (ct_hbm, ct_s, chunk * val, 0),
        )):
            copies.append(
                pltpu.make_async_copy(
                    source.at[:, first + c * size : first + (c + 1) * size],
                    target.at[:, c * size : (c + 1) * size],
                    sems.at[c * 4 + t],
                )
            )
    copies.append(pltpu.make_async_copy(kt_hbm, kt_s, sems.at[CHUNKS * 4]))
    for copy in copies:
        copy.start()
    pad = jnp.zeros((*qf_s.shape[:2], qf_s.shape[2] - full), BF16)
    qf_s[:, :, full:] = pad
    live = live_rows(rlen, parts, rows)
    for j in range(heads):
        if j % chunk == 0:
            for copy in copies[j // chunk * 4 : j // chunk * 4 + 4]:
                copy.wait()
        at = j * width
        wk_j = wk_s[:, j * nope : (j + 1) * nope]
        q_lat = dot(q_s[:, at : at + nope], wk_j, NT).astype(BF16)
        q_rope = q_s[:, at + nope : at + width]
        cols = slice(j * val, (j + 1) * val)
        g_lat = (dot(ct_s[:, cols], wv_s[:, cols], NT) * live).astype(BF16)
        for r in range(parts):
            here = slice(r * rows, (r + 1) * rows)
            there = slice(j * rows, (j + 1) * rows)
            qf_s[r, there, :lat] = q_lat[here]
            qf_s[r, there, lat:full] = q_rope[here]
            gl_s[r, there, :] = g_lat[here]
    copies[-1].wait()
    block, keys = heads * rows, kt_s.shape[2]
    raw = [dot(qf_s[r], kt_s[r]) for r in range(parts)]
    heard = [dot(gl_s[r], kt_s[r, :lat]) for r in range(parts)]
    for r in range(parts):
        place = lax.broadcasted_iota(jnp.int32, (rows, keys), 0)
        key = lax.broadcasted_iota(jnp.int32, (rows, keys), 1)
        own = key - (prows + r * rows)
        valid = (key < plen[r]) | ((own >= 0) & (own <= place))
        bias = jnp.where(valid, 0.0, -jnp.inf)
        scores = (raw[r] * scale).reshape(heads, rows, keys) + bias[None]
        scores = scores.reshape(block, keys)
        expo = jnp.exp(scores - jnp.max(scores, axis=1, keepdims=True))
        weights = expo * (1.0 / jnp.sum(expo, axis=1, keepdims=True))
        inner = jnp.sum(weights * heard[r], axis=1, keepdims=True)
        w_ref[r] = weights.astype(BF16)
        gs_ref[r] = (weights * (heard[r] - inner) * scale).astype(BF16)
    mine = None
    for r in range(parts):
        grad_k = dot(qf_s[r], gs_ref[r], TN)
        grad_v = dot(gl_s[r], w_ref[r], TN)
        low = grad_k[:lat] + grad_v
        cols = slice(r * prows, (r + 1) * prows)
        gk_ref[:lat, cols] = low[:, :prows].astype(BF16)
        gk_ref[lat:, cols] = grad_k[lat:full, :prows].astype(BF16)
        part = jnp.concatenate([low[:, prows:], grad_k[lat:full, prows:]], axis=0)
        mine = part if mine is None else mine + part
    go_ref[...] = mine


def values_kernel(sizes, rlen, wv_ref, wk_ref, k_ref, w_ref, gs_ref, out_ref, gq_ref):
    parts, rows, heads, nope, rope, val, lat, prows = sizes
    full = lat + rope
    wv, wk = wv_ref[...], wk_ref[...]
    live = live_rows(rlen, parts, rows)
    lows = [dot(w_ref[r], k_ref[r, :, :lat]).astype(BF16) for r in range(parts)]
    grads = [dot(gs_ref[r], k_ref[r]).astype(BF16) for r in range(parts)]
    pieces = []
    for j in range(heads):
        there = slice(j * rows, (j + 1) * rows)
        low = jnp.concatenate([one[there] for one in lows], axis=0)
        grad = jnp.concatenate([one[there] for one in grads], axis=0)
        heard = dot(low, wv[:, j * val : (j + 1) * val]) * live
        out_ref[:, j * val : (j + 1) * val] = heard.astype(BF16)
        pieces.append(dot(grad[:, :lat], wk[:, j * nope : (j + 1) * nope]).astype(BF16))
        pieces.append(grad[:, lat:full])
    gq_ref[...] = jnp.concatenate(pieces, axis=1)


def attend(plen, rlen, queries, cotangent, weights, k, kt, full, prows, nope):
    parts, keys, wide = k.shape
    lat = weights.shape[0]
    rope = full - lat
    width = nope + rope
    tokens = queries.shape[0]
    heads = queries.shape[1] // width
    val = cotangent.shape[1] // heads
    rows = tokens // parts
    vs = VALUE_HEADS
    sizes = (parts, rows, heads, nope, rope, val, lat, prows)
    w_shape = jax.ShapeDtypeStruct((parts, heads * rows, keys), BF16)

    def specs(count):
        steps = heads // count
        return (
            pl.BlockSpec((lat, count * val), lambda i, *_: (0, i)),
            pl.BlockSpec((lat, count * nope), lambda i, *_: (0, i + steps)),
            pl.BlockSpec((tokens, count * width), lambda i, *_: (0, i)),
            pl.BlockSpec((tokens, count * val), lambda i, *_: (0, i)),
            pl.BlockSpec((parts, count * rows, keys), lambda i, *_: (0, i, 0)),
        )

    raw = pl.BlockSpec(memory_space=pl.ANY)
    w_spec = specs(heads)[-1]
    params = pltpu.CompilerParams(
        dimension_semantics=("arbitrary",), vmem_limit_bytes=30 << 20
    )
    queries, cotangent, weights, k, kt = (
        pltpu.with_memory_space_constraint(a, pltpu.HBM)
        for a in (queries, cotangent, weights, k, kt)
    )
    grad_key, grad_own, soft, grad_s = pl.pallas_call(
        functools.partial(scores_kernel, sizes),
        out_shape=(
            jax.ShapeDtypeStruct((full, parts * prows), BF16),
            jax.ShapeDtypeStruct((full, tokens), F32),
            w_shape,
            w_shape,
        ),
        grid_spec=pltpu.PrefetchScalarGridSpec(
            num_scalar_prefetch=2,
            grid=(1,),
            in_specs=[raw] * 4,
            out_specs=[whole(full, parts * prows), whole(full, tokens), w_spec, w_spec],
            scratch_shapes=[
                pltpu.VMEM(queries.shape, BF16),
                pltpu.VMEM(cotangent.shape, BF16),
                pltpu.VMEM((lat, heads * val), BF16),
                pltpu.VMEM((lat, heads * nope), BF16),
                pltpu.VMEM(kt.shape, BF16),
                pltpu.VMEM((parts, heads * rows, wide), BF16),
                pltpu.VMEM((parts, heads * rows, lat), BF16),
                pltpu.SemaphoreType.DMA((CHUNKS * 4 + 1,)),
            ],
        ),
        compiler_params=params,
        cost_estimate=pl.CostEstimate(
            flops=2 * tokens * heads * (2 * lat * nope + keys * (2 * full + 2 * lat)),
            transcendentals=tokens * heads * keys,
            bytes_accessed=8 << 20,
        ),
        name="scores",
    )(plen, rlen, queries, cotangent, weights, kt)
    wv_spec, wk_spec, q_spec, v_spec, w_spec = specs(vs)
    sizes = (parts, rows, vs, nope, rope, val, lat, prows)
    attended, grad_query = pl.pallas_call(
        functools.partial(values_kernel, sizes),
        out_shape=(
            jax.ShapeDtypeStruct((tokens, heads * val), BF16),
            jax.ShapeDtypeStruct((tokens, heads * width), BF16),
        ),
        grid_spec=pltpu.PrefetchScalarGridSpec(
            num_scalar_prefetch=1,
            grid=(heads // vs,),
            in_specs=[wv_spec, wk_spec, whole(*k.shape), w_spec, w_spec],
            out_specs=[v_spec, q_spec],
        ),
        compiler_params=params,
        cost_estimate=pl.CostEstimate(
            flops=2 * tokens * heads * (2 * lat * nope + keys * (full + lat)),
            transcendentals=0,
            bytes_accessed=8 << 20,
        ),
        name="values",
    )(rlen, weights, weights, k, soft, grad_s)
    return attended, grad_query, grad_key, grad_own


def slots_kernel(place, in_ref, out_ref, acc_s):
    senders, _, wide = in_ref.shape
    takers, _, lanes = out_ref.shape
    parts = wide // lanes
    acc_s[...] = jnp.zeros_like(acc_s)
    for s in range(senders):
        for r in range(parts):
            to = place[s * parts + r]
            acc_s[to] += in_ref[s, :, r * lanes : (r + 1) * lanes].astype(F32)
    out_ref[...] = acc_s[:takers].astype(BF16)


def by_slot(place, in_row, takers, lanes):
    shape = (takers, in_row.shape[1], lanes)
    return pl.pallas_call(
        slots_kernel,
        out_shape=jax.ShapeDtypeStruct(shape, BF16),
        grid_spec=pltpu.PrefetchScalarGridSpec(
            num_scalar_prefetch=1,
            grid=(1,),
            in_specs=[whole(*in_row.shape)],
            out_specs=whole(*shape),
            scratch_shapes=[pltpu.VMEM((takers + 1, *shape[1:]), F32)],
        ),
        compiler_params=pltpu.CompilerParams(vmem_limit_bytes=8 << 20),
        name="by_slot",
    )(place, in_row)


def side_of(axis):
    return math.isqrt(lax.axis_size(axis))


def rows_of(side):
    return [[y * side + z for z in range(side)] for y in range(side)]


def columns_of(side):
    return [[y * side + z for y in range(side)] for z in range(side)]


def exchange(tiles, axis, groups=None):
    return lax.all_to_all(tiles, axis, 0, 0, axis_index_groups=groups, tiled=True)


def to_all(array, count, axis, groups=None):
    return exchange(jnp.broadcast_to(array, (count, *array.shape)), axis, groups)


def body(
    queries,
    resp_latent,
    prompt_latent,
    up_keys,
    up_values,
    cotangent,
    prompt_len,
    resp_len,
    resp_count,
    owner,
):
    head_devices = lax.axis_size("head")
    side = side_of("resp")
    along_z, along_y = rows_of(side), columns_of(side)
    my_index = lax.axis_index("resp")
    my_y, my_z = my_index // side, my_index % side
    head_index = lax.axis_index("head")
    heads, nope, lat_piece = up_keys.shape
    val = up_values.shape[2]
    resp_total = resp_len.shape[0]
    per_device = resp_total // lax.axis_size("resp")
    _, prompt_rows, full = prompt_latent.shape
    share = full // head_devices

    tiles = jnp.concatenate([up_values, jnp.swapaxes(up_keys, 1, 2)], axis=0)
    got = to_all(tiles, side, "resp", along_z)
    stripes = jnp.moveaxis(got, 2, 1).reshape(side * lat_piece, -1)
    weights = lax.all_gather(
        stripes, "resp", axis=0, tiled=True, axis_index_groups=along_y
    )
    cols = jnp.swapaxes(prompt_latent[0], 0, 1)
    cols = lax.dynamic_slice_in_dim(cols, head_index * share, share, 0)
    cols, _ = lax.optimization_barrier((cols, got[0, 0, 0]))
    column_prompts = to_all(cols, side, "resp", along_y)

    starts = jnp.cumsum(resp_count) - resp_count
    numbers = jnp.arange(resp_total, dtype=jnp.int32)
    prompt_of = jnp.sum((starts[None, :] <= numbers[:, None]).astype(jnp.int32), axis=1) - 1
    chosen = prompt_of[:, None] == jnp.arange(prompt_len.shape[0], dtype=jnp.int32)[None, :]
    slot_of = jnp.sum(jnp.where(chosen, owner[None, :], 0), axis=1)
    plen_of = jnp.sum(jnp.where(chosen, prompt_len[None, :], 0), axis=1)
    first = my_index * per_device
    plen_mine = lax.dynamic_slice_in_dim(plen_of, first, per_device)
    rlen_mine = lax.dynamic_slice_in_dim(resp_len, first, per_device)
    slots_mine = lax.dynamic_slice_in_dim(slot_of, first, per_device)

    by_place = slot_of.reshape(side, side, per_device)
    row_slots = lax.dynamic_index_in_dim(by_place, my_y, 0, keepdims=False)
    wanted = jnp.take(column_prompts, (row_slots // side).reshape(-1), axis=0)
    wanted = wanted.reshape(side, per_device, share, prompt_rows)
    arrived = exchange(wanted, "resp", along_z)
    mine = (slots_mine % side)[None, :] == jnp.arange(side, dtype=jnp.int32)[:, None]
    fetched = jnp.sum(
        jnp.where(mine[:, :, None, None], arrived, 0).astype(F32), axis=0
    ).astype(BF16)
    k_prompt = to_all(fetched, head_devices, "head")
    k_prompt = jnp.moveaxis(k_prompt, 0, 1).reshape(per_device, full, prompt_rows)
    k_own = jnp.swapaxes(resp_latent, 0, 1)

    place = jnp.where(row_slots % side == my_z, row_slots // side, side).reshape(-1)
    k_prompt, place = lax.optimization_barrier((k_prompt, place))
    k, kt = both_keys(k_prompt, k_own)

    attended, grad_query, grad_key, grad_own = attend(
        plen_mine, rlen_mine, queries, cotangent, weights, k, kt, full, prompt_rows, nope
    )
    grad_own = lax.psum_scatter(grad_own, "head", scatter_dimension=0, tiled=True)
    grad_own = jnp.swapaxes(grad_own, 0, 1)
    by_head = exchange(grad_key.reshape(head_devices, share, -1), "head")
    grad_prompt = jnp.sum(by_head.astype(F32), axis=0).astype(BF16)
    grad_prompt, attended = lax.optimization_barrier((grad_prompt, attended))
    in_row = to_all(grad_prompt, side, "resp", along_z)
    to_owner = by_slot(place, in_row, side, prompt_rows)
    at_owner = exchange(to_owner, "resp", along_y)
    at_owner = jnp.sum(at_owner.astype(F32), axis=0)
    return (attended, grad_query, grad_own, jnp.swapaxes(at_owner, 0, 1)[None])


def solution(mesh):
    placed = (
        P("resp", "head"),
        P("resp", None),
        P("resp", None, None),
        P("head", None, "resp"),
        P("head", "resp", None),
        P("resp", "head"),
        P(),
        P(),
        P(),
        P(),
    )
    return jax.shard_map(
        body,
        mesh=mesh,
        in_specs=placed,
        out_specs=(
            P("resp", "head"),
            P("resp", "head"),
            P("resp", "head"),
            P("resp", None, "head"),
        ),
        check_vma=False,
    )
```

```python
import functools
import math

import jax
import jax.numpy as jnp
from jax import lax
from jax.experimental import pallas as pl
from jax.experimental.pallas import tpu as pltpu
from jax.sharding import PartitionSpec as P

F32, BF16 = jnp.float32, jnp.bfloat16
CHUNKS, VALUE_HEADS = 4, 8
NT, TN = ((1,), (1,)), ((0,), (0,))


def dot(left, right, dims=((1,), (0,))):
    return lax.dot_general(left, right, (dims, ((), ())), preferred_element_type=F32)


def whole(*shape):
    return pl.BlockSpec(shape, lambda i, *_: (0,) * len(shape))


def keys_kernel(kp_ref, ko_ref, k_ref, kt_ref):
    parts, full, prows = kp_ref.shape
    own = ko_ref[...]
    own_rows = jnp.transpose(own)
    for r in range(parts):
        cols = kp_ref[r]
        kt_ref[r] = jnp.zeros(kt_ref.shape[1:], BF16)
        kt_ref[r, :full, :prows] = cols
        kt_ref[r, :full, prows:] = own
        k_ref[r] = jnp.zeros(k_ref.shape[1:], BF16)
        k_ref[r, :prows, :full] = jnp.transpose(cols)
        k_ref[r, prows:, :full] = own_rows


def both_keys(k_prompt, k_own):
    parts, full, prows = k_prompt.shape
    keys = prows + k_own.shape[1]
    wide = -(-full // 128) * 128
    shapes = (parts, keys, wide), (parts, wide, keys)
    return pl.pallas_call(
        keys_kernel,
        out_shape=tuple(jax.ShapeDtypeStruct(s, BF16) for s in shapes),
        grid=(1,),
        in_specs=[whole(*k_prompt.shape), whole(*k_own.shape)],
        out_specs=[whole(*s) for s in shapes],
        compiler_params=pltpu.CompilerParams(vmem_limit_bytes=12 << 20),
        name="both_keys",
    )(k_prompt, k_own)


def live_rows(rlen, parts, rows):
    spot = lax.broadcasted_iota(jnp.int32, (parts * rows, 1), 0)
    live = jnp.zeros(spot.shape, F32)
    for r in range(parts):
        alive = (spot >= r * rows) & (spot < r * rows + rlen[r])
        live = jnp.where(alive, 1.0, live)
    return live


def scores_kernel(
    sizes, plen, rlen, q_hbm, ct_hbm, w_hbm, kt_hbm,
    gk_ref, go_ref, w_ref, gs_ref,
    q_s, ct_s, wv_s, wk_s, kt_s, qf_s, gl_s, sems,
):
    parts, rows, heads, nope, rope, val, lat, prows = sizes
    full, width = lat + rope, nope + rope
    scale = 1.0 / math.sqrt(width)
    chunk = heads // CHUNKS
    copies = []
    for c in range(CHUNKS):
        for t, (source, target, size, first) in enumerate((
            (w_hbm, wk_s, chunk * nope, heads * val),
            (q_hbm, q_s, chunk * width, 0),
            (w_hbm, wv_s, chunk * val, 0),
            (ct_hbm, ct_s, chunk * val, 0),
        )):
            copies.append(
                pltpu.make_async_copy(
                    source.at[:, first + c * size : first + (c + 1) * size],
                    target.at[:, c * size : (c + 1) * size],
                    sems.at[c * 4 + t],
                )
            )
    copies.append(pltpu.make_async_copy(kt_hbm, kt_s, sems.at[CHUNKS * 4]))
    for copy in copies:
        copy.start()
    pad = jnp.zeros((*qf_s.shape[:2], qf_s.shape[2] - full), BF16)
    qf_s[:, :, full:] = pad
    live = live_rows(rlen, parts, rows)
    for j in range(heads):
        if j % chunk == 0:
            for copy in copies[j // chunk * 4 : j // chunk * 4 + 4]:
                copy.wait()
        at = j * width
        wk_j = wk_s[:, j * nope : (j + 1) * nope]
        q_lat = dot(q_s[:, at : at + nope], wk_j, NT).astype(BF16)
        q_rope = q_s[:, at + nope : at + width]
        cols = slice(j * val, (j + 1) * val)
        g_lat = (dot(ct_s[:, cols], wv_s[:, cols], NT) * live).astype(BF16)
        for r in range(parts):
            here = slice(r * rows, (r + 1) * rows)
            there = slice(j * rows, (j + 1) * rows)
            qf_s[r, there, :lat] = q_lat[here]
            qf_s[r, there, lat:full] = q_rope[here]
            gl_s[r, there, :] = g_lat[here]
    copies[-1].wait()
    block, keys = heads * rows, kt_s.shape[2]
    raw = [dot(qf_s[r], kt_s[r]) for r in range(parts)]
    heard = [dot(gl_s[r], kt_s[r, :lat]) for r in range(parts)]
    for r in range(parts):
        place = lax.broadcasted_iota(jnp.int32, (rows, keys), 0)
        key = lax.broadcasted_iota(jnp.int32, (rows, keys), 1)
        own = key - (prows + r * rows)
        valid = (key < plen[r]) | ((own >= 0) & (own <= place))
        bias = jnp.where(valid, 0.0, -jnp.inf)
        scores = (raw[r] * scale).reshape(heads, rows, keys) + bias[None]
        scores = scores.reshape(block, keys)
        expo = jnp.exp(scores - jnp.max(scores, axis=1, keepdims=True))
        weights = expo * (1.0 / jnp.sum(expo, axis=1, keepdims=True))
        inner = jnp.sum(weights * heard[r], axis=1, keepdims=True)
        w_ref[r] = weights.astype(BF16)
        gs_ref[r] = (weights * (heard[r] - inner) * scale).astype(BF16)
    mine = None
    for r in range(parts):
        grad_k = dot(qf_s[r], gs_ref[r], TN)
        grad_v = dot(gl_s[r], w_ref[r], TN)
        low = grad_k[:lat] + grad_v
        cols = slice(r * prows, (r + 1) * prows)
        gk_ref[:lat, cols] = low[:, :prows].astype(BF16)
        gk_ref[lat:, cols] = grad_k[lat:full, :prows].astype(BF16)
        part = jnp.concatenate([low[:, prows:], grad_k[lat:full, prows:]], axis=0)
        mine = part if mine is None else mine + part
    go_ref[...] = mine


def values_kernel(sizes, rlen, wv_ref, wk_ref, k_ref, w_ref, gs_ref, out_ref, gq_ref):
    parts, rows, heads, nope, rope, val, lat, prows = sizes
    full = lat + rope
    wv, wk = wv_ref[...], wk_ref[...]
    live = live_rows(rlen, parts, rows)
    lows = [dot(w_ref[r], k_ref[r, :, :lat]).astype(BF16) for r in range(parts)]
    grads = [dot(gs_ref[r], k_ref[r]).astype(BF16) for r in range(parts)]
    pieces = []
    for j in range(heads):
        there = slice(j * rows, (j + 1) * rows)
        low = jnp.concatenate([one[there] for one in lows], axis=0)
        grad = jnp.concatenate([one[there] for one in grads], axis=0)
        heard = dot(low, wv[:, j * val : (j + 1) * val]) * live
        out_ref[:, j * val : (j + 1) * val] = heard.astype(BF16)
        pieces.append(dot(grad[:, :lat], wk[:, j * nope : (j + 1) * nope]).astype(BF16))
        pieces.append(grad[:, lat:full])
    gq_ref[...] = jnp.concatenate(pieces, axis=1)


def attend(plen, rlen, queries, cotangent, weights, k, kt, full, prows, nope):
    parts, keys, wide = k.shape
    lat = weights.shape[0]
    rope = full - lat
    width = nope + rope
    tokens = queries.shape[0]
    heads = queries.shape[1] // width
    val = cotangent.shape[1] // heads
    rows = tokens // parts
    vs = VALUE_HEADS
    sizes = (parts, rows, heads, nope, rope, val, lat, prows)
    w_shape = jax.ShapeDtypeStruct((parts, heads * rows, keys), BF16)

    def specs(count):
        steps = heads // count
        return (
            pl.BlockSpec((lat, count * val), lambda i, *_: (0, i)),
            pl.BlockSpec((lat, count * nope), lambda i, *_: (0, i + steps)),
            pl.BlockSpec((tokens, count * width), lambda i, *_: (0, i)),
            pl.BlockSpec((tokens, count * val), lambda i, *_: (0, i)),
            pl.BlockSpec((parts, count * rows, keys), lambda i, *_: (0, i, 0)),
        )

    raw = pl.BlockSpec(memory_space=pl.ANY)
    w_spec = specs(heads)[-1]
    params = pltpu.CompilerParams(
        dimension_semantics=("arbitrary",), vmem_limit_bytes=30 << 20
    )
    queries, cotangent, weights, k, kt = (
        pltpu.with_memory_space_constraint(a, pltpu.HBM)
        for a in (queries, cotangent, weights, k, kt)
    )
    grad_key, grad_own, soft, grad_s = pl.pallas_call(
        functools.partial(scores_kernel, sizes),
        out_shape=(
            jax.ShapeDtypeStruct((full, parts * prows), BF16),
            jax.ShapeDtypeStruct((full, tokens), F32),
            w_shape,
            w_shape,
        ),
        grid_spec=pltpu.PrefetchScalarGridSpec(
            num_scalar_prefetch=2,
            grid=(1,),
            in_specs=[raw] * 4,
            out_specs=[whole(full, parts * prows), whole(full, tokens), w_spec, w_spec],
            scratch_shapes=[
                pltpu.VMEM(queries.shape, BF16),
                pltpu.VMEM(cotangent.shape, BF16),
                pltpu.VMEM((lat, heads * val), BF16),
                pltpu.VMEM((lat, heads * nope), BF16),
                pltpu.VMEM(kt.shape, BF16),
                pltpu.VMEM((parts, heads * rows, wide), BF16),
                pltpu.VMEM((parts, heads * rows, lat), BF16),
                pltpu.SemaphoreType.DMA((CHUNKS * 4 + 1,)),
            ],
        ),
        compiler_params=params,
        cost_estimate=pl.CostEstimate(
            flops=2 * tokens * heads * (2 * lat * nope + keys * (2 * full + 2 * lat)),
            transcendentals=tokens * heads * keys,
            bytes_accessed=8 << 20,
        ),
        name="scores",
    )(plen, rlen, queries, cotangent, weights, kt)
    wv_spec, wk_spec, q_spec, v_spec, w_spec = specs(vs)
    sizes = (parts, rows, vs, nope, rope, val, lat, prows)
    attended, grad_query = pl.pallas_call(
        functools.partial(values_kernel, sizes),
        out_shape=(
            jax.ShapeDtypeStruct((tokens, heads * val), BF16),
            jax.ShapeDtypeStruct((tokens, heads * width), BF16),
        ),
        grid_spec=pltpu.PrefetchScalarGridSpec(
            num_scalar_prefetch=1,
            grid=(heads // vs,),
            in_specs=[wv_spec, wk_spec, whole(*k.shape), w_spec, w_spec],
            out_specs=[v_spec, q_spec],
        ),
        compiler_params=params,
        cost_estimate=pl.CostEstimate(
            flops=2 * tokens * heads * (2 * lat * nope + keys * (full + lat)),
            transcendentals=0,
            bytes_accessed=8 << 20,
        ),
        name="values",
    )(rlen, weights, weights, k, soft, grad_s)
    return attended, grad_query, grad_key, grad_own


def slots_kernel(place, in_ref, out_ref, acc_s):
    senders, _, wide = in_ref.shape
    takers, _, lanes = out_ref.shape
    parts = wide // lanes
    acc_s[...] = jnp.zeros_like(acc_s)
    for s in range(senders):
        for r in range(parts):
            to = place[s * parts + r]
            acc_s[to] += in_ref[s, :, r * lanes : (r + 1) * lanes].astype(F32)
    out_ref[...] = acc_s[:takers].astype(BF16)


def by_slot(place, in_row, takers, lanes):
    shape = (takers, in_row.shape[1], lanes)
    return pl.pallas_call(
        slots_kernel,
        out_shape=jax.ShapeDtypeStruct(shape, BF16),
        grid_spec=pltpu.PrefetchScalarGridSpec(
            num_scalar_prefetch=1,
            grid=(1,),
            in_specs=[whole(*in_row.shape)],
            out_specs=whole(*shape),
            scratch_shapes=[pltpu.VMEM((takers + 1, *shape[1:]), F32)],
        ),
        compiler_params=pltpu.CompilerParams(vmem_limit_bytes=8 << 20),
        name="by_slot",
    )(place, in_row)


def side_of(axis):
    return math.isqrt(lax.axis_size(axis))


def rows_of(side):
    return [[y * side + z for z in range(side)] for y in range(side)]


def columns_of(side):
    return [[y * side + z for y in range(side)] for z in range(side)]


def exchange(tiles, axis, groups=None):
    return lax.all_to_all(tiles, axis, 0, 0, axis_index_groups=groups, tiled=True)


def to_all(array, count, axis, groups=None):
    return exchange(jnp.broadcast_to(array, (count, *array.shape)), axis, groups)


def body(
    queries,
    resp_latent,
    prompt_latent,
    up_keys,
    up_values,
    cotangent,
    prompt_len,
    resp_len,
    resp_count,
    owner,
):
    head_devices = lax.axis_size("head")
    side = side_of("resp")
    along_z, along_y = rows_of(side), columns_of(side)
    my_index = lax.axis_index("resp")
    my_y, my_z = my_index // side, my_index % side
    head_index = lax.axis_index("head")
    heads, nope, lat_piece = up_keys.shape
    val = up_values.shape[2]
    resp_total = resp_len.shape[0]
    per_device = resp_total // lax.axis_size("resp")
    _, prompt_rows, full = prompt_latent.shape
    share = full // head_devices

    tiles = jnp.concatenate([up_values, jnp.swapaxes(up_keys, 1, 2)], axis=0)
    got = to_all(tiles, side, "resp", along_z)
    stripes = jnp.moveaxis(got, 2, 1).reshape(side * lat_piece, -1)
    weights = lax.all_gather(
        stripes, "resp", axis=0, tiled=True, axis_index_groups=along_y
    )
    cols = jnp.swapaxes(prompt_latent[0], 0, 1)
    cols = lax.dynamic_slice_in_dim(cols, head_index * share, share, 0)
    cols, _ = lax.optimization_barrier((cols, got[0, 0, 0]))
    column_prompts = to_all(cols, side, "resp", along_y)

    starts = jnp.cumsum(resp_count) - resp_count
    numbers = jnp.arange(resp_total, dtype=jnp.int32)
    prompt_of = jnp.sum((starts[None, :] <= numbers[:, None]).astype(jnp.int32), axis=1) - 1
    chosen = prompt_of[:, None] == jnp.arange(prompt_len.shape[0], dtype=jnp.int32)[None, :]
    slot_of = jnp.sum(jnp.where(chosen, owner[None, :], 0), axis=1)
    plen_of = jnp.sum(jnp.where(chosen, prompt_len[None, :], 0), axis=1)
    first = my_index * per_device
    plen_mine = lax.dynamic_slice_in_dim(plen_of, first, per_device)
    rlen_mine = lax.dynamic_slice_in_dim(resp_len, first, per_device)
    slots_mine = lax.dynamic_slice_in_dim(slot_of, first, per_device)

    by_place = slot_of.reshape(side, side, per_device)
    row_slots = lax.dynamic_index_in_dim(by_place, my_y, 0, keepdims=False)
    wanted = jnp.take(column_prompts, (row_slots // side).reshape(-1), axis=0)
    wanted = wanted.reshape(side, per_device, share, prompt_rows)
    arrived = exchange(wanted, "resp", along_z)
    mine = (slots_mine % side)[None, :] == jnp.arange(side, dtype=jnp.int32)[:, None]
    fetched = jnp.sum(
        jnp.where(mine[:, :, None, None], arrived, 0).astype(F32), axis=0
    ).astype(BF16)
    k_prompt = to_all(fetched, head_devices, "head")
    k_prompt = jnp.moveaxis(k_prompt, 0, 1).reshape(per_device, full, prompt_rows)
    k_own = jnp.swapaxes(resp_latent, 0, 1)

    in_column = lax.dynamic_index_in_dim(by_place, my_z, 1, keepdims=False)
    place = jnp.where(in_column // side == my_y, in_column % side, side).reshape(-1)
    k_prompt, place = lax.optimization_barrier((k_prompt, place))
    k, kt = both_keys(k_prompt, k_own)

    attended, grad_query, grad_key, grad_own = attend(
        plen_mine, rlen_mine, queries, cotangent, weights, k, kt, full, prompt_rows, nope
    )
    grad_own = lax.psum_scatter(grad_own, "head", scatter_dimension=0, tiled=True)
    grad_own = jnp.swapaxes(grad_own, 0, 1)
    by_head = exchange(grad_key.reshape(head_devices, share, -1), "head")
    grad_prompt = jnp.sum(by_head.astype(F32), axis=0).astype(BF16)
    grad_prompt, attended = lax.optimization_barrier((grad_prompt, attended))
    column = to_all(grad_prompt, side, "resp", along_y)
    to_owner = by_slot(place, column, side, prompt_rows)
    at_owner = exchange(to_owner, "resp", along_z)
    at_owner = jnp.sum(at_owner.astype(F32), axis=0)
    return (attended, grad_query, grad_own, jnp.swapaxes(at_owner, 0, 1)[None])


def solution(mesh):
    placed = (
        P("resp", "head"),
        P("resp", None),
        P("resp", None, None),
        P("head", None, "resp"),
        P("head", "resp", None),
        P("resp", "head"),
        P(),
        P(),
        P(),
        P(),
    )
    return jax.shard_map(
        body,
        mesh=mesh,
        in_specs=placed,
        out_specs=(
            P("resp", "head"),
            P("resp", "head"),
            P("resp", "head"),
            P("resp", None, "head"),
        ),
        check_vma=False,
    )
```

```python
import functools
import math

import jax
import jax.numpy as jnp
from jax import lax
from jax.experimental import pallas as pl
from jax.experimental.pallas import tpu as pltpu
from jax.sharding import PartitionSpec as P

F32, BF16 = jnp.float32, jnp.bfloat16
CHUNKS, VALUE_HEADS = 4, 8
NT, TN = ((1,), (1,)), ((0,), (0,))


def dot(left, right, dims=((1,), (0,))):
    return lax.dot_general(left, right, (dims, ((), ())), preferred_element_type=F32)


def whole(*shape):
    return pl.BlockSpec(shape, lambda i, *_: (0,) * len(shape))


def keys_kernel(kp_ref, ko_ref, k_ref, kt_ref):
    parts, full, prows = kp_ref.shape
    own = ko_ref[...]
    own_rows = jnp.transpose(own)
    for r in range(parts):
        cols = kp_ref[r]
        kt_ref[r] = jnp.zeros(kt_ref.shape[1:], BF16)
        kt_ref[r, :full, :prows] = cols
        kt_ref[r, :full, prows:] = own
        k_ref[r] = jnp.zeros(k_ref.shape[1:], BF16)
        k_ref[r, :prows, :full] = jnp.transpose(cols)
        k_ref[r, prows:, :full] = own_rows


def both_keys(k_prompt, k_own):
    parts, full, prows = k_prompt.shape
    keys = prows + k_own.shape[1]
    wide = -(-full // 128) * 128
    shapes = (parts, keys, wide), (parts, wide, keys)
    return pl.pallas_call(
        keys_kernel,
        out_shape=tuple(jax.ShapeDtypeStruct(s, BF16) for s in shapes),
        grid=(1,),
        in_specs=[whole(*k_prompt.shape), whole(*k_own.shape)],
        out_specs=[whole(*s) for s in shapes],
        compiler_params=pltpu.CompilerParams(vmem_limit_bytes=12 << 20),
        name="both_keys",
    )(k_prompt, k_own)


def live_rows(rlen, parts, rows):
    spot = lax.broadcasted_iota(jnp.int32, (parts * rows, 1), 0)
    live = jnp.zeros(spot.shape, F32)
    for r in range(parts):
        alive = (spot >= r * rows) & (spot < r * rows + rlen[r])
        live = jnp.where(alive, 1.0, live)
    return live


def scores_kernel(
    sizes, plen, rlen, q_hbm, ct_hbm, w_hbm, kt_hbm,
    gk_ref, go_ref, w_ref, gs_ref,
    q_s, ct_s, wv_s, wk_s, kt_s, qf_s, gl_s, sems,
):
    parts, rows, heads, nope, rope, val, lat, prows = sizes
    full, width = lat + rope, nope + rope
    scale = 1.0 / math.sqrt(width)
    chunk = heads // CHUNKS
    copies = []
    for c in range(CHUNKS):
        for t, (source, target, size, first) in enumerate((
            (w_hbm, wk_s, chunk * nope, heads * val),
            (q_hbm, q_s, chunk * width, 0),
            (w_hbm, wv_s, chunk * val, 0),
            (ct_hbm, ct_s, chunk * val, 0),
        )):
            copies.append(
                pltpu.make_async_copy(
                    source.at[:, first + c * size : first + (c + 1) * size],
                    target.at[:, c * size : (c + 1) * size],
                    sems.at[c * 4 + t],
                )
            )
    copies.append(pltpu.make_async_copy(kt_hbm, kt_s, sems.at[CHUNKS * 4]))
    for copy in copies:
        copy.start()
    pad = jnp.zeros((*qf_s.shape[:2], qf_s.shape[2] - full), BF16)
    qf_s[:, :, full:] = pad
    live = live_rows(rlen, parts, rows)
    for j in range(heads):
        if j % chunk == 0:
            for copy in copies[j // chunk * 4 : j // chunk * 4 + 4]:
                copy.wait()
        at = j * width
        wk_j = wk_s[:, j * nope : (j + 1) * nope]
        q_lat = dot(q_s[:, at : at + nope], wk_j, NT).astype(BF16)
        q_rope = q_s[:, at + nope : at + width]
        cols = slice(j * val, (j + 1) * val)
        g_lat = (dot(ct_s[:, cols], wv_s[:, cols], NT) * live).astype(BF16)
        for r in range(parts):
            here = slice(r * rows, (r + 1) * rows)
            there = slice(j * rows, (j + 1) * rows)
            qf_s[r, there, :lat] = q_lat[here]
            qf_s[r, there, lat:full] = q_rope[here]
            gl_s[r, there, :] = g_lat[here]
    copies[-1].wait()
    block, keys = heads * rows, kt_s.shape[2]
    raw = [dot(qf_s[r], kt_s[r]) for r in range(parts)]
    heard = [dot(gl_s[r], kt_s[r, :lat]) for r in range(parts)]
    for r in range(parts):
        place = lax.broadcasted_iota(jnp.int32, (rows, keys), 0)
        key = lax.broadcasted_iota(jnp.int32, (rows, keys), 1)
        own = key - (prows + r * rows)
        valid = (key < plen[r]) | ((own >= 0) & (own <= place))
        bias = jnp.where(valid, 0.0, -jnp.inf)
        scores = (raw[r] * scale).reshape(heads, rows, keys) + bias[None]
        scores = scores.reshape(block, keys)
        expo = jnp.exp(scores - jnp.max(scores, axis=1, keepdims=True))
        weights = expo * (1.0 / jnp.sum(expo, axis=1, keepdims=True))
        inner = jnp.sum(weights * heard[r], axis=1, keepdims=True)
        w_ref[r] = weights.astype(BF16)
        gs_ref[r] = (weights * (heard[r] - inner) * scale).astype(BF16)
    mine = None
    for r in range(parts):
        grad_k = dot(qf_s[r], gs_ref[r], TN)
        grad_v = dot(gl_s[r], w_ref[r], TN)
        low = grad_k[:lat] + grad_v
        cols = slice(r * prows, (r + 1) * prows)
        gk_ref[:lat, cols] = low[:, :prows].astype(BF16)
        gk_ref[lat:, cols] = grad_k[lat:full, :prows].astype(BF16)
        part = jnp.concatenate([low[:, prows:], grad_k[lat:full, prows:]], axis=0)
        mine = part if mine is None else mine + part
    go_ref[...] = mine


def values_kernel(sizes, rlen, wv_ref, wk_ref, k_ref, w_ref, gs_ref, out_ref, gq_ref):
    parts, rows, heads, nope, rope, val, lat, prows = sizes
    full = lat + rope
    wv, wk = wv_ref[...], wk_ref[...]
    live = live_rows(rlen, parts, rows)
    lows = [dot(w_ref[r], k_ref[r, :, :lat]).astype(BF16) for r in range(parts)]
    grads = [dot(gs_ref[r], k_ref[r]).astype(BF16) for r in range(parts)]
    pieces = []
    for j in range(heads):
        there = slice(j * rows, (j + 1) * rows)
        low = jnp.concatenate([one[there] for one in lows], axis=0)
        grad = jnp.concatenate([one[there] for one in grads], axis=0)
        heard = dot(low, wv[:, j * val : (j + 1) * val]) * live
        out_ref[:, j * val : (j + 1) * val] = heard.astype(BF16)
        pieces.append(dot(grad[:, :lat], wk[:, j * nope : (j + 1) * nope]).astype(BF16))
        pieces.append(grad[:, lat:full])
    gq_ref[...] = jnp.concatenate(pieces, axis=1)


def attend(plen, rlen, queries, cotangent, weights, k, kt, full, prows, nope):
    parts, keys, wide = k.shape
    lat = weights.shape[0]
    rope = full - lat
    width = nope + rope
    tokens = queries.shape[0]
    heads = queries.shape[1] // width
    val = cotangent.shape[1] // heads
    rows = tokens // parts
    vs = VALUE_HEADS
    sizes = (parts, rows, heads, nope, rope, val, lat, prows)
    w_shape = jax.ShapeDtypeStruct((parts, heads * rows, keys), BF16)

    def specs(count):
        steps = heads // count
        return (
            pl.BlockSpec((lat, count * val), lambda i, *_: (0, i)),
            pl.BlockSpec((lat, count * nope), lambda i, *_: (0, i + steps)),
            pl.BlockSpec((tokens, count * width), lambda i, *_: (0, i)),
            pl.BlockSpec((tokens, count * val), lambda i, *_: (0, i)),
            pl.BlockSpec((parts, count * rows, keys), lambda i, *_: (0, i, 0)),
        )

    raw = pl.BlockSpec(memory_space=pl.ANY)
    w_spec = specs(heads)[-1]
    params = pltpu.CompilerParams(
        dimension_semantics=("arbitrary",), vmem_limit_bytes=30 << 20
    )
    queries, cotangent, weights, k, kt = (
        pltpu.with_memory_space_constraint(a, pltpu.HBM)
        for a in (queries, cotangent, weights, k, kt)
    )
    grad_key, grad_own, soft, grad_s = pl.pallas_call(
        functools.partial(scores_kernel, sizes),
        out_shape=(
            jax.ShapeDtypeStruct((full, parts * prows), BF16),
            jax.ShapeDtypeStruct((full, tokens), F32),
            w_shape,
            w_shape,
        ),
        grid_spec=pltpu.PrefetchScalarGridSpec(
            num_scalar_prefetch=2,
            grid=(1,),
            in_specs=[raw] * 4,
            out_specs=[whole(full, parts * prows), whole(full, tokens), w_spec, w_spec],
            scratch_shapes=[
                pltpu.VMEM(queries.shape, BF16),
                pltpu.VMEM(cotangent.shape, BF16),
                pltpu.VMEM((lat, heads * val), BF16),
                pltpu.VMEM((lat, heads * nope), BF16),
                pltpu.VMEM(kt.shape, BF16),
                pltpu.VMEM((parts, heads * rows, wide), BF16),
                pltpu.VMEM((parts, heads * rows, lat), BF16),
                pltpu.SemaphoreType.DMA((CHUNKS * 4 + 1,)),
            ],
        ),
        compiler_params=params,
        cost_estimate=pl.CostEstimate(
            flops=2 * tokens * heads * (2 * lat * nope + keys * (2 * full + 2 * lat)),
            transcendentals=tokens * heads * keys,
            bytes_accessed=8 << 20,
        ),
        name="scores",
    )(plen, rlen, queries, cotangent, weights, kt)
    wv_spec, wk_spec, q_spec, v_spec, w_spec = specs(vs)
    sizes = (parts, rows, vs, nope, rope, val, lat, prows)
    attended, grad_query = pl.pallas_call(
        functools.partial(values_kernel, sizes),
        out_shape=(
            jax.ShapeDtypeStruct((tokens, heads * val), BF16),
            jax.ShapeDtypeStruct((tokens, heads * width), BF16),
        ),
        grid_spec=pltpu.PrefetchScalarGridSpec(
            num_scalar_prefetch=1,
            grid=(heads // vs,),
            in_specs=[wv_spec, wk_spec, whole(*k.shape), w_spec, w_spec],
            out_specs=[v_spec, q_spec],
        ),
        compiler_params=params,
        cost_estimate=pl.CostEstimate(
            flops=2 * tokens * heads * (2 * lat * nope + keys * (full + lat)),
            transcendentals=0,
            bytes_accessed=8 << 20,
        ),
        name="values",
    )(rlen, weights, weights, k, soft, grad_s)
    return attended, grad_query, grad_key, grad_own


def slots_kernel(place, in_ref, out_ref, acc_s):
    senders, _, wide = in_ref.shape
    takers, _, lanes = out_ref.shape
    parts = wide // lanes
    acc_s[...] = jnp.zeros_like(acc_s)
    for s in range(senders):
        for r in range(parts):
            to = place[s * parts + r]
            acc_s[to] += in_ref[s, :, r * lanes : (r + 1) * lanes].astype(F32)
    out_ref[...] = acc_s[:takers].astype(BF16)


def by_slot(place, in_row, takers, lanes):
    shape = (takers, in_row.shape[1], lanes)
    return pl.pallas_call(
        slots_kernel,
        out_shape=jax.ShapeDtypeStruct(shape, BF16),
        grid_spec=pltpu.PrefetchScalarGridSpec(
            num_scalar_prefetch=1,
            grid=(1,),
            in_specs=[whole(*in_row.shape)],
            out_specs=whole(*shape),
            scratch_shapes=[pltpu.VMEM((takers + 1, *shape[1:]), F32)],
        ),
        compiler_params=pltpu.CompilerParams(vmem_limit_bytes=8 << 20),
        name="by_slot",
    )(place, in_row)


def side_of(axis):
    return math.isqrt(lax.axis_size(axis))


def rows_of(side):
    return [[y * side + z for z in range(side)] for y in range(side)]


def columns_of(side):
    return [[y * side + z for y in range(side)] for z in range(side)]


def exchange(tiles, axis, groups=None):
    return lax.all_to_all(tiles, axis, 0, 0, axis_index_groups=groups, tiled=True)


def to_all(array, count, axis, groups=None):
    return exchange(jnp.broadcast_to(array, (count, *array.shape)), axis, groups)


def body(
    queries,
    resp_latent,
    prompt_latent,
    up_keys,
    up_values,
    cotangent,
    prompt_len,
    resp_len,
    resp_count,
    owner,
):
    head_devices = lax.axis_size("head")
    side = side_of("resp")
    along_z, along_y = rows_of(side), columns_of(side)
    my_index = lax.axis_index("resp")
    my_y, my_z = my_index // side, my_index % side
    head_index = lax.axis_index("head")
    heads, nope, lat_piece = up_keys.shape
    val = up_values.shape[2]
    resp_total = resp_len.shape[0]
    per_device = resp_total // lax.axis_size("resp")
    _, prompt_rows, full = prompt_latent.shape
    share = full // head_devices

    tiles = jnp.concatenate([up_values, jnp.swapaxes(up_keys, 1, 2)], axis=0)
    got = to_all(tiles, side, "resp", along_z)
    stripes = jnp.moveaxis(got, 2, 1).reshape(side * lat_piece, -1)
    weights = lax.all_gather(
        stripes, "resp", axis=0, tiled=True, axis_index_groups=along_y
    )
    cols = jnp.swapaxes(prompt_latent[0], 0, 1)
    cols = lax.dynamic_slice_in_dim(cols, head_index * share, share, 0)
    cols, _ = lax.optimization_barrier((cols, got[0, 0, 0]))
    column_prompts = to_all(cols, side, "resp", along_y)

    starts = jnp.cumsum(resp_count) - resp_count
    numbers = jnp.arange(resp_total, dtype=jnp.int32)
    prompt_of = jnp.sum((starts[None, :] <= numbers[:, None]).astype(jnp.int32), axis=1) - 1
    chosen = prompt_of[:, None] == jnp.arange(prompt_len.shape[0], dtype=jnp.int32)[None, :]
    slot_of = jnp.sum(jnp.where(chosen, owner[None, :], 0), axis=1)
    plen_of = jnp.sum(jnp.where(chosen, prompt_len[None, :], 0), axis=1)
    first = my_index * per_device
    plen_mine = lax.dynamic_slice_in_dim(plen_of, first, per_device)
    rlen_mine = lax.dynamic_slice_in_dim(resp_len, first, per_device)
    slots_mine = lax.dynamic_slice_in_dim(slot_of, first, per_device)

    by_place = slot_of.reshape(side, side, per_device)
    row_slots = lax.dynamic_index_in_dim(by_place, my_y, 0, keepdims=False)
    wanted = jnp.take(column_prompts, (row_slots // side).reshape(-1), axis=0)
    wanted = wanted.reshape(side, per_device, share, prompt_rows)
    arrived = exchange(wanted, "resp", along_z)
    mine = (slots_mine % side)[None, :] == jnp.arange(side, dtype=jnp.int32)[:, None]
    fetched = jnp.sum(
        jnp.where(mine[:, :, None, None], arrived, 0).astype(F32), axis=0
    ).astype(BF16)
    k_prompt = to_all(fetched, head_devices, "head")
    k_prompt = jnp.moveaxis(k_prompt, 0, 1).reshape(per_device, full, prompt_rows)
    k_own = jnp.swapaxes(resp_latent, 0, 1)

    in_column = lax.dynamic_index_in_dim(by_place, my_z, 1, keepdims=False)
    place = jnp.where(in_column // side == my_y, in_column % side, side).reshape(-1)
    k_prompt, place = lax.optimization_barrier((k_prompt, place))
    k, kt = both_keys(k_prompt, k_own)

    attended, grad_query, grad_key, grad_own = attend(
        plen_mine, rlen_mine, queries, cotangent, weights, k, kt, full, prompt_rows, nope
    )
    grad_own = lax.psum_scatter(grad_own, "head", scatter_dimension=0, tiled=True)
    grad_own = jnp.swapaxes(grad_own, 0, 1)
    by_head = exchange(grad_key.reshape(head_devices, share, -1), "head")
    grad_prompt = jnp.sum(by_head.astype(F32), axis=0).astype(BF16)
    column = to_all(grad_prompt, side, "resp", along_y)
    place, attended = lax.optimization_barrier((place, attended))
    to_owner = by_slot(place, column, side, prompt_rows)
    at_owner = exchange(to_owner, "resp", along_z)
    at_owner = jnp.sum(at_owner.astype(F32), axis=0)
    return (attended, grad_query, grad_own, jnp.swapaxes(at_owner, 0, 1)[None])


def solution(mesh):
    placed = (
        P("resp", "head"),
        P("resp", None),
        P("resp", None, None),
        P("head", None, "resp"),
        P("head", "resp", None),
        P("resp", "head"),
        P(),
        P(),
        P(),
        P(),
    )
    return jax.shard_map(
        body,
        mesh=mesh,
        in_specs=placed,
        out_specs=(
            P("resp", "head"),
            P("resp", "head"),
            P("resp", "head"),
            P("resp", None, "head"),
        ),
        check_vma=False,
    )
```
